128 devices in a mesh: gz: 2 (over x_lo), gx: 2 (over core), gy: 32 (over z, y, x_hi).
Axes of the slice: x: 4 (x_hi: 2, x_lo: 2; x = x_hi * 2 + x_lo), y: 4, z: 4, core: 2. Of those that a mesh axis runs over, the one named last changes fastest.
Arguments:
- initial_field: float32 [128, 16, 4096], P('gz', 'gx', 'gy'), may hold values from -36 to 36
- plane_coupling: float32 [128, 16, 4096], P('gz', 'gx', 'gy'), may hold values from 0.06 to 0.24
- line_coupling: float32 [128, 16, 4096], P('gz', 'gx', 'gy'), may hold values from 1000 to 8000
- source: float32 [128, 16, 4096], P('gz', 'gx', 'gy'), may hold values from -4 to 4, as said below
- shift_table: float32 [8], replicated, may hold values from 0.5 to 1
- shift_index: int32 [4], replicated, may hold values from 0 to 7
Outputs:
- heated: float32 [128, 16, 4096], P('gz', 'gx', 'gy')
The draws below stay inside these ranges and needn't reach their ends.
Inputs may be any that keep to these rules, and one draw needn't show every extreme that they name: `shift_index`: one table row for each half-step. A heat source.
All inputs are finite; a program needn't handle non-finite values.
Results may differ from the reference program's by a relative error of at most 0.0003.
Values sent between devices are 32-bit elements; how exact they have to be, the bound alone decides.
A program may use at most 64 MiB of HBM per device.

```python
import math
import jax
import jax.numpy as jnp
from jax import lax

SHIFTS = 8
HALF = 4
NX = 16
NY = 4096
NZ = 128


def draw_source(key, part):
    values = jnp.clip(jax.random.normal(key, (NZ, NX, NY), jnp.float32), -4.0, 4.0)
    return values


def place_ends(entries, rng, least, top_value):
    dims = entries.shape
    place = [jax.random.randint(jax.random.fold_in(rng, axis), (), 0, dims[axis]) for axis in range(len(dims))]
    entries = entries.at[tuple(place)].set(least)
    longest = dims.index(max(dims))
    place[longest] = (place[longest] + 1) % dims[longest]
    return entries.at[tuple(place)].set(top_value)


def block_scale(stream_key, dims, shards, low, top_value):
    level = 1.0
    for axis_at, blocks in shards:
        draws = jax.random.uniform(jax.random.fold_in(jax.random.fold_in(stream_key, 6), axis_at), (blocks,), jnp.float32, low / len(shards), top_value / len(shards))
        level = level * jnp.repeat(jnp.exp(draws), dims[axis_at] // blocks).reshape((-1,) + (1,) * (len(dims) - 1 - axis_at))
    return level


def centred(stream_key, dims, scale, most, shards=(), kind=jnp.bfloat16):
    loudness = block_scale(stream_key, dims, shards, -0.22, 0.18) if shards else 1.0
    array = jax.random.normal(stream_key, dims, jnp.float32) * scale * loudness
    return jnp.minimum(jnp.maximum(array, -most), most).astype(kind)


def setup_inputs(seed: int = 0) -> dict:
    seeds = jax.random.split(jax.random.key(seed), 7)
    initial_field = centred(seeds[0], (NZ, NX, NY), 6.0, 36.0, ((0, 2), (1, 2), (2, 32)), jnp.float32)
    plane_coupling = jnp.clip(jnp.exp(math.log(0.24) - 1.3862944 * jax.random.uniform(seeds[1], (NZ, NX, NY), jnp.float32) ** block_scale(seeds[1], (NZ, NX, NY), ((0, 2), (1, 2), (2, 32)), -0.2, 0.2)), 0.06, 0.24)
    line_coupling = jnp.clip(jnp.exp(math.log(8000.0) - 2.0794415 * jax.random.uniform(seeds[2], (NZ, NX, NY), jnp.float32) ** block_scale(seeds[2], (NZ, NX, NY), ((0, 2), (1, 2), (2, 32)), -0.2, 0.2)), 1000.0, 8000.0)
    source = draw_source(jax.random.fold_in(seeds[6], 71), 0)
    shift_table = jnp.clip(jax.random.uniform(seeds[4], (SHIFTS,), jnp.float32, 0.5, 1.0), 0.5, 1.0)
    shift_index = place_ends(jax.random.randint(seeds[5], (HALF,), 0, SHIFTS), jax.random.fold_in(seeds[5], 1), 0, SHIFTS - 1).astype(jnp.int32)
    return {"initial_field": initial_field, "plane_coupling": plane_coupling, "line_coupling": line_coupling, "source": source, "shift_table": shift_table, "shift_index": shift_index}


def lookup(shift_table, table_row):
    table_slots = jnp.arange(shift_table.shape[0], dtype=jnp.int32)
    return jnp.sum(jnp.where(table_slots == table_row, shift_table, jnp.zeros_like(shift_table)))


def plane_apply(current, coupling):
    padded = jnp.pad(current, ((0, 0), (1, 1), (1, 1)))
    beside_all = padded[:, 2:, 1:-1] + padded[:, :-2, 1:-1] + padded[:, 1:-1, 2:] + padded[:, 1:-1, :-2]
    return coupling * (beside_all - 4.0 * current)


def line_solve(explicit, line_coupling, shift_value):
    scaled = shift_value * line_coupling
    center = 1.0 + 2.0 * scaled

    def forward(previous, inputs):
        before_c, before_d = previous
        coupling, middle, right_side = inputs
        pivot_value = middle + coupling * before_c
        next_c = -coupling / pivot_value
        next_d = (right_side + coupling * before_d) / pivot_value
        return (next_c, next_d), (next_c, next_d)

    zero_plane = jnp.zeros_like(explicit[0])
    final_state, factors = lax.scan(forward, (zero_plane, zero_plane), (scaled, center, explicit))

    def backward(later_value, inputs):
        ratio, offset = inputs
        own_value = offset - ratio * later_value
        return own_value, own_value

    final_value, solved = lax.scan(backward, zero_plane, factors, reverse=True)
    return solved


def reference(initial_field, plane_coupling, line_coupling, source, shift_table, shift_index):
    current = initial_field
    for half_step in range(HALF):
        shift_value = lookup(shift_table, shift_index[half_step])
        explicit = current + shift_value * (plane_apply(current, plane_coupling) + source)
        current = line_solve(explicit, line_coupling, shift_value)
    return current
```

```python
import functools

import jax
import jax.numpy as jnp
from jax import lax
from jax.experimental import pallas as pl
from jax.experimental.pallas import tpu as pltpu
from jax.sharding import PartitionSpec as P

HALF = 4
NJ = 64
MESH = pl.DeviceIdType.MESH
U, PC, SRC, LC = range(4)
LC_FILL = 4000.0


def kernel(
    ny,
    u_hbm, pc_hbm, lc_hbm, src_hbm, table, rows,
    out_ref,
    raw, fac, prv, quo, dsc, mid, gtx, grx, dtx, drx,
    own_pk, own_rx, halo_pk, halo_rx, est, efac, eprv, equo, eds, erx,
    load_sem, raw_sem, own_sem, halo_sem, g_sem, d_sem, e_sem,
):
    gz, gx, gy = lax.axis_index("gz"), lax.axis_index("gx"), lax.axis_index("gy")
    has_left, has_right = gy > 0, gy < ny - 1
    y_left, y_right = lax.rem(gy + ny - 1, ny), lax.rem(gy + 1, ny)
    lane = lax.broadcasted_iota(jnp.int32, (8, 128), 1)
    row = lax.broadcasted_iota(jnp.int32, (8, 128), 0)
    base = 64 * gx + 32 * gz
    ones = jnp.full((8, 128), 1.0, jnp.float32)
    zero = jnp.zeros((8, 128), jnp.float32)

    def zof(j):
        return jnp.where(gz == 0, j, NJ - 1 - j)

    def remote(src, dst, send, recv, dev):
        return pltpu.make_async_remote_copy(
            src_ref=src, dst_ref=dst, send_sem=send, recv_sem=recv, device_id=dev, device_id_type=MESH
        )

    def roll(v, amount, axis=1):
        return pltpu.roll(v, amount, axis)

    loads = [
        pltpu.make_async_copy(ref, raw.at[a, gx], load_sem.at[a])
        for a, ref in ((LC, lc_hbm), (U, u_hbm), (PC, pc_hbm), (SRC, src_hbm))
    ]
    for c in loads:
        c.start()
    barrier = pltpu.get_barrier_semaphore()

    def hello(dev):
        pl.semaphore_signal(barrier, inc=1, device_id=dev, device_id_type=MESH)

    hello((gz, 1 - gx, gy))
    hello((1 - gz, gx, gy))
    hello((1 - gz, 1 - gx, gy))

    @pl.when((gx == 0) & has_left)
    def _():
        for z in range(2):
            for x in range(2):
                hello((z, x, y_left))

    @pl.when((gx == 1) & has_right)
    def _():
        for z in range(2):
            for x in range(2):
                hello((z, x, y_right))

    for c in loads:
        c.wait()

    def pack(g, _):
        for a in range(4):
            own_l, own_r, hl, hr = [zero, zero], [zero, zero], zero, zero
            for i in range(32):
                v = raw[a, gx, zof(g * 32 + i)]
                h, jj = i // 16, i % 16
                at = (4 + 8 * jj) % 128
                m8 = ((lane - at) & 127) < 8
                own_l[h] = jnp.where(m8, roll(v, at), own_l[h])
                own_r[h] = jnp.where(m8, roll(v, (at - 120) % 128), own_r[h])
                at = (12 + 4 * i) % 128
                hl = jnp.where(((lane - at) & 127) < 4, roll(v, at) if at else v, hl)
                at = 4 * i
                hr = jnp.where(((lane - at) & 127) < 4, roll(v, (at - 124) % 128), hr)
            for h in range(2):
                own_pk[0, a, 2 * g + h] = roll(own_l[h], base)
                own_pk[1, a, 2 * g + h] = roll(own_r[h], base)
            halo_pk[0, a, g] = roll(hl, base)
            halo_pk[1, a, g] = roll(hr, base)
        return 0

    lax.fori_loop(0, 2, pack, 0)
    for a in range(4):
        for g in range(4):
            own_rx[gx, gz, a, g] = own_pk[gx, a, g]

    pl.semaphore_wait(barrier, 3 + 2 * has_left.astype(jnp.int32) + 2 * has_right.astype(jnp.int32))

    raw_cp = [
        remote(raw.at[a, gx], raw.at[a, gx], raw_sem.at[0, a], raw_sem.at[1, a], (gz, 1 - gx, gy))
        for a in (LC, U, PC, SRC)
    ]
    for c in raw_cp:
        c.start()
    def halo_l():
        return [
            remote(halo_pk.at[0], halo_rx.at[gx, gz], halo_sem.at[0, 0, z], halo_sem.at[1, gx, gz], (z, 1, y_left))
            for z in range(2)
        ]

    def halo_r():
        return [
            remote(halo_pk.at[1], halo_rx.at[gx, gz], halo_sem.at[0, 1, z], halo_sem.at[1, gx, gz], (z, 0, y_right))
            for z in range(2)
        ]

    @pl.when(has_left)
    def _():
        for c in halo_l():
            c.start()

    @pl.when(has_right)
    def _():
        for c in halo_r():
            c.start()

    own_cp = [
        remote(own_pk.at[1 - gx], own_rx.at[gx, gz], own_sem.at[0, 0, 0], own_sem.at[1, gx, gz], (gz, 1 - gx, gy)),
        remote(own_pk.at[0], own_rx.at[gx, gz], own_sem.at[0, 0, 1], own_sem.at[1, gx, gz], (1 - gz, 0, gy)),
        remote(own_pk.at[1], own_rx.at[gx, gz], own_sem.at[0, 1, 0], own_sem.at[1, gx, gz], (1 - gz, 1, gy)),
    ]
    for c in own_cp:
        c.start()

    inv = []
    for k in range(HALF):
        shift = jnp.float32(0.0)
        for i in range(table.shape[0]):
            shift = shift + jnp.where(rows[k] == i, table[i], 0.0)
        inv.append(1.0 / jnp.full((8, 128), shift, jnp.float32))

    def factors(load_lc, store):
        def block(b, carry):
            ps, ds, rs = carry
            ps, ds, rs = list(ps), list(ds), list(rs)
            for i in range(4):
                j = b * 4 + i
                t_line = 1.0 / load_lc(j)
                for k in range(HALF):
                    old, r_old = ps[k], rs[k]
                    ds[k] = ds[k] + (t_line * inv[k]) * old
                    ps[k] = old + ds[k]
                    rs[k] = 1.0 / ps[k]
                    store(k, j, t_line * old, old, r_old * rs[k])
            return tuple(ps), tuple(ds), tuple(rs)

        start = (ones,) * HALF
        return lax.fori_loop(0, NJ // 4, block, (start, start, start))

    def main_factors(t):
        def store(k, j, f, p, q):
            z = zof(j)
            fac[k, t, z] = f
            prv[k, t, z] = p
            quo[k, t, z] = q

        ps, ds, rs = factors(lambda j: raw[LC, t, zof(j)], store)
        for k in range(HALF):
            mid[0, k, t] = rs[k]
            gtx[k, t] = ds[k] * rs[k]

    main_factors(gx)
    for c in raw_cp:
        c.wait()
    main_factors(1 - gx)
    g_cp = remote(gtx, grx, g_sem.at[0], g_sem.at[1], (1 - gz, gx, gy))
    g_cp.start()

    def forward_main(k):
        def block(b, totals):
            totals = list(totals)
            for i in range(4):
                z = zof(b * 4 + i)
                us = [raw[U, 0, z], raw[U, 1, z]]
                down = [roll(u, 1, 0) for u in us]
                up = [roll(u, 7, 0) for u in us]
                low = [jnp.where(row == 0, 0.0, down[0]), jnp.where(row == 0, down[0], down[1])]
                high = [jnp.where(row == 7, up[1], up[0]), jnp.where(row == 7, 0.0, up[1])]
                for t in range(2):
                    beside = (low[t] + high[t]) + (roll(us[t], 1) + roll(us[t], 127))
                    e = inv[k] * us[t] + raw[PC, t, z] * (beside - 4.0 * us[t]) + raw[SRC, t, z]
                    totals[t] = totals[t] + fac[k, t, z] * e
                    dsc[t, z] = totals[t]
            return tuple(totals)

        totals = lax.fori_loop(0, NJ // 4, block, (zero, zero))
        for t in range(2):
            dtx[k, t] = totals[t] * mid[0, k, t]
        cp = remote(dtx.at[k], drx.at[k], d_sem.at[0, k], d_sem.at[1, k], (1 - gz, gx, gy))
        cp.start()
        return cp

    def backward_main(k):
        last = zof(NJ - 1)
        ys = []
        for t in range(2):
            y = (dtx[k, t] + (1.0 - gtx[k, t]) * drx[k, t]) * mid[1, k, t]
            raw[U, t, last] = prv[k, t, last] * y
            ys.append(y)

        def block(b, ys):
            ys = list(ys)
            for i in range(7):
                z = zof(NJ - 2 - (b * 7 + i))
                for t in range(2):
                    ys[t] = ys[t] + dsc[t, z] * quo[k, t, z]
                    raw[U, t, z] = prv[k, t, z] * ys[t]
            return tuple(ys)

        lax.fori_loop(0, 9, block, tuple(ys))

    quads = [(x, z) for x in range(2) for z in range(2)]
    fills = {U: 0.0, PC: 0.0, SRC: 0.0, LC: LC_FILL}

    def unpack_own():
        def block(g, _):
            for jj in range(16):
                masks = [((lane - (64 * x + 32 * z + 4 + 8 * jj)) & 127) < 8 for x, z in quads]
                for a in range(4):
                    v = jnp.full((8, 128), fills[a], jnp.float32)
                    for (x, z), m in zip(quads, masks):
                        v = jnp.where(m, own_rx[x, z, a, g], v)
                    est[a, g * 16 + jj] = roll(v, (-8 * jj) % 128) if jj else v
            return 0

        lax.fori_loop(0, 4, block, 0)

    def unpack_halo():
        shifted = lane - 12 * gx

        def block(g, _):
            for jj in range(32):
                masks = [((shifted - (64 * x + 32 * z + 4 * jj)) & 127) < 4 for x, z in quads]
                m_all = (shifted & 31) < 4
                for a in range(4):
                    v = zero
                    for (x, z), m in zip(quads, masks):
                        v = jnp.where(m, halo_rx[x, z, a, g], v)
                    v = roll(v, (-4 * jj) % 128) if jj else v
                    est[a, g * 32 + jj] = jnp.where(m_all, v, est[a, g * 32 + jj])
            return 0

        lax.fori_loop(0, 2, block, 0)

    def edge_factors():
        def store(k, j, f, p, q):
            efac[k, j] = f
            eprv[k, j] = p
            equo[k, j] = q

        return factors(lambda j: est[LC, j], store)

    def other_half(v):
        return jnp.where((lane & 32) == 0, roll(v, 96), roll(v, 32))

    def edge_step(k, delta, recip):
        outer_low = (row == 0) & (lane < 64)
        outer_high = (row == 7) & (lane >= 64)

        def fwd(b, total):
            for i in range(4):
                j = b * 4 + i
                u = est[U, j]
                cross = roll(u, 64)
                low = jnp.where(outer_low, 0.0, roll(jnp.where(row == 7, cross, u), 1, 0))
                high = jnp.where(outer_high, 0.0, roll(jnp.where(row == 0, cross, u), 7, 0))
                beside = (low + high) + (roll(u, 1) + roll(u, 127))
                e = inv[k] * u + est[PC, j] * (beside - 4.0 * u) + est[SRC, j]
                total = total + efac[k, j] * e
                eds[j] = total
            return total

        total = lax.fori_loop(0, NJ // 4, fwd, zero)
        d = total * recip
        g = delta * recip
        last_p = eprv[k, NJ - 1]
        y = (d + (1.0 - g) * other_half(d)) / ((g + other_half(g) * (1.0 - g)) * last_p)
        est[U, NJ - 1] = last_p * y

        def back(b, y):
            for i in range(7):
                j = NJ - 2 - (b * 7 + i)
                y = y + eds[j] * equo[k, j]
                est[U, j] = eprv[k, j] * y
            return y

        lax.fori_loop(0, 9, back, y)

    cp = forward_main(0)
    for c in own_cp:
        c.wait_send()
    for x, z in quads:

        @pl.when((x != gx) | (z != gz))
        def _():
            remote(own_rx.at[x, z], own_rx.at[x, z], own_sem.at[0, 0, 0], own_sem.at[1, x, z], (gz, 1 - gx, gy)).wait_recv()

    unpack_own()
    g_cp.wait()
    for k in range(HALF):
        for t in range(2):
            g = gtx[k, t]
            mid[1, k, t] = 1.0 / ((g + grx[k, t] * (1.0 - g)) * prv[k, t, zof(NJ - 1)])
    cp.wait()
    backward_main(0)
    cp = forward_main(1)
    cp.wait()
    backward_main(1)
    cp = forward_main(2)

    @pl.when(has_left)
    def _():
        for c in halo_l():
            c.wait_send()

    @pl.when(has_right)
    def _():
        for c in halo_r():
            c.wait_send()

    @pl.when(((gx == 0) & has_left) | ((gx == 1) & has_right))
    def _():
        for x, z in quads:
            remote(halo_rx.at[x, z], halo_rx.at[x, z], halo_sem.at[0, 0, 0], halo_sem.at[1, x, z], (gz, 1 - gx, gy)).wait_recv()
        unpack_halo()

    e_ps, e_ds, e_rs = edge_factors()
    cp.wait()
    backward_main(2)
    cp = forward_main(3)
    for k in range(HALF):
        edge_step(k, e_ds[k], e_rs[k])
    e_cp = remote(est.at[U], erx, e_sem.at[0], e_sem.at[1], (gz, 1 - gx, gy))
    e_cp.start()
    cp.wait()
    backward_main(3)
    e_cp.wait()

    def shift_of(side):
        return (120 * side - (base + 4 + 4 * side) + 4 * side + 256) % 128

    mine, other = shift_of(gx), shift_of(1 - gx)
    first, last = lane < 4, lane >= 124
    mine_mask = (first & (gx == 0)) | (last & (gx == 1))
    other_mask = (first & (gx == 1)) | (last & (gx == 0))

    def merge(b, _):
        for i in range(8):
            j = b * 8 + i
            z = zof(j)
            v = jnp.where(mine_mask, roll(est[U, j], mine), raw[U, gx, z])
            out_ref[z] = jnp.where(other_mask, roll(erx[j], other), v)
        return 0

    lax.fori_loop(0, NJ // 8, merge, 0)


def solution(mesh):
    ny = mesh.shape["gy"]
    block = (NJ, 8, 128)
    vmem = lambda *s: pltpu.VMEM((*s, 8, 128), jnp.float32)

    def on_device(u, pc, lc, src, table, rows):
        hbm = pl.BlockSpec(memory_space=pl.ANY)
        smem = pl.BlockSpec(memory_space=pltpu.SMEM)
        return pl.pallas_call(
            functools.partial(kernel, ny),
            out_shape=jax.ShapeDtypeStruct(block, jnp.float32),
            in_specs=[hbm, hbm, hbm, hbm, smem, smem],
            out_specs=pl.BlockSpec(memory_space=pltpu.VMEM),
            scratch_shapes=[
                vmem(4, 2, NJ),
                vmem(HALF, 2, NJ), vmem(HALF, 2, NJ), vmem(HALF, 2, NJ),
                vmem(2, NJ), vmem(2, HALF, 2),
                vmem(HALF, 2), vmem(HALF, 2), vmem(HALF, 2), vmem(HALF, 2),
                vmem(2, 4, 4), vmem(2, 2, 4, 4), vmem(2, 4, 2), vmem(2, 2, 4, 2),
                vmem(4, NJ), vmem(HALF, NJ), vmem(HALF, NJ), vmem(HALF, NJ),
                vmem(NJ), vmem(NJ),
                pltpu.SemaphoreType.DMA((4,)),
                pltpu.SemaphoreType.DMA((2, 4)),
                pltpu.SemaphoreType.DMA((2, 2, 2)),
                pltpu.SemaphoreType.DMA((2, 2, 2)),
                pltpu.SemaphoreType.DMA((2,)),
                pltpu.SemaphoreType.DMA((2, HALF)),
                pltpu.SemaphoreType.DMA((2,)),
            ],
            compiler_params=pltpu.CompilerParams(collective_id=0, has_side_effects=True),
        )(u, pc, lc, src, table, rows)

    split = P("gz", "gx", "gy")
    return jax.shard_map(
        on_device, mesh=mesh, in_specs=(split,) * 4 + (P(), P()), out_specs=split, check_vma=False
    )
```

```python
import functools

import jax
import jax.numpy as jnp
from jax import lax
from jax.experimental import pallas as pl
from jax.experimental.pallas import tpu as pltpu
from jax.sharding import PartitionSpec as P

HALF = 4
NJ = 64
MESH = pl.DeviceIdType.MESH
U, PC, SRC, LC = range(4)
LC_FILL = 4000.0


def kernel(
    ny,
    u_hbm, pc_hbm, lc_hbm, src_hbm, table, rows,
    out_ref,
    raw, fac, prv, quo, dsc, mid, gtx, grx, dtx, drx,
    own_pk, own_rx, halo_pk, halo_rx, est, efac, eprv, equo, eds, erx,
    load_sem, raw_sem, own_sem, halo_sem, g_sem, d_sem, e_sem,
):
    gz, gx, gy = lax.axis_index("gz"), lax.axis_index("gx"), lax.axis_index("gy")
    has_left, has_right = gy > 0, gy < ny - 1
    y_left, y_right = lax.rem(gy + ny - 1, ny), lax.rem(gy + 1, ny)
    lane = lax.broadcasted_iota(jnp.int32, (8, 128), 1)
    row = lax.broadcasted_iota(jnp.int32, (8, 128), 0)
    base = 64 * gx + 32 * gz
    ones = jnp.full((8, 128), 1.0, jnp.float32)
    zero = jnp.zeros((8, 128), jnp.float32)

    def zof(j):
        return jnp.where(gz == 0, j, NJ - 1 - j)

    def remote(src, dst, send, recv, dev):
        return pltpu.make_async_remote_copy(
            src_ref=src, dst_ref=dst, send_sem=send, recv_sem=recv, device_id=dev, device_id_type=MESH
        )

    def roll(v, amount, axis=1):
        return pltpu.roll(v, amount, axis)

    loads = [
        pltpu.make_async_copy(ref, raw.at[a, gx], load_sem.at[a])
        for a, ref in ((LC, lc_hbm), (U, u_hbm), (PC, pc_hbm), (SRC, src_hbm))
    ]
    for c in loads:
        c.start()
    barrier = pltpu.get_barrier_semaphore()

    def hello(dev):
        pl.semaphore_signal(barrier, inc=1, device_id=dev, device_id_type=MESH)

    hello((gz, 1 - gx, gy))
    hello((1 - gz, gx, gy))
    hello((1 - gz, 1 - gx, gy))

    @pl.when((gx == 0) & has_left)
    def _():
        for z in range(2):
            for x in range(2):
                hello((z, x, y_left))

    @pl.when((gx == 1) & has_right)
    def _():
        for z in range(2):
            for x in range(2):
                hello((z, x, y_right))

    for c in loads:
        c.wait()

    low_half, even = (lane & 7) < 4, (lane & 8) == 0

    def pack(g, _):
        for a in range(4):
            left, right = [], []
            for h in range(2):
                both = []
                for q in range(2):
                    v = zero
                    for b in range(8):
                        at = 16 * b
                        w = roll(raw[a, gx, zof(g * 32 + h * 16 + q * 8 + b)], (at + 8) % 128)
                        v = w if b == 0 else jnp.where((lane >= at) & (lane < at + 16), w, v)
                    both.append(v)
                left.append(jnp.where(even, roll(both[0], 120), both[1]))
                right.append(jnp.where(even, both[0], roll(both[1], 8)))
            for h in range(2):
                own_pk[0, a, 2 * g + h] = roll(left[h], base + 4)
                own_pk[1, a, 2 * g + h] = roll(right[h], base + 4)
            halo_pk[0, a, g] = roll(jnp.where(low_half, left[0], roll(left[1], 4)), base + 12)
            halo_pk[1, a, g] = roll(jnp.where(low_half, roll(right[0], 124), right[1]), base)
        return 0

    def octet(jj):
        return 8 * (2 * jj if jj < 8 else 2 * (jj - 8) + 1)

    with jax.named_scope("pack"):
        lax.fori_loop(0, 2, pack, 0)
    for a in range(4):
        for g in range(4):
            own_rx[gx, gz, a, g] = own_pk[gx, a, g]

    inv = []
    for k in range(HALF):
        shift = jnp.float32(0.0)
        for i in range(table.shape[0]):
            shift = shift + jnp.where(rows[k] == i, table[i], 0.0)
        inv.append(1.0 / jnp.full((8, 128), shift, jnp.float32))

    def factors(load_lc, store):
        def block(b, carry):
            ps, ds, rs = carry
            ps, ds, rs = list(ps), list(ds), list(rs)
            for i in range(4):
                j = b * 4 + i
                t_line = 1.0 / load_lc(j)
                for k in range(HALF):
                    old, r_old = ps[k], rs[k]
                    ds[k] = ds[k] + (t_line * inv[k]) * old
                    ps[k] = old + ds[k]
                    rs[k] = 1.0 / ps[k]
                    store(k, j, t_line * old, old, r_old * rs[k])
            return tuple(ps), tuple(ds), tuple(rs)

        start = (ones,) * HALF
        return lax.fori_loop(0, NJ // 4, block, (start, start, start))

    def main_factors(t):
        def store(k, j, f, p, q):
            z = zof(j)
            fac[k, t, z] = f
            prv[k, t, z] = p
            quo[k, t, z] = q

        ps, ds, rs = factors(lambda j: raw[LC, t, zof(j)], store)
        for k in range(HALF):
            mid[0, k, t] = rs[k]
            gtx[k, t] = ds[k] * rs[k]

    with jax.named_scope("fac0"):
        main_factors(gx)

    with jax.named_scope("wait_barrier"):
        pl.semaphore_wait(barrier, 3 + 2 * has_left.astype(jnp.int32) + 2 * has_right.astype(jnp.int32))

    raw_cp = [
        remote(raw.at[a, gx], raw.at[a, gx], raw_sem.at[0, a], raw_sem.at[1, a], (gz, 1 - gx, gy))
        for a in (LC, U, PC, SRC)
    ]
    for c in raw_cp:
        c.start()
    def halo_l():
        return [
            remote(halo_pk.at[0], halo_rx.at[gx, gz], halo_sem.at[0, 0, z], halo_sem.at[1, gx, gz], (z, 1, y_left))
            for z in range(2)
        ]

    def halo_r():
        return [
            remote(halo_pk.at[1], halo_rx.at[gx, gz], halo_sem.at[0, 1, z], halo_sem.at[1, gx, gz], (z, 0, y_right))
            for z in range(2)
        ]

    @pl.when(has_left)
    def _():
        for c in halo_l():
            c.start()

    @pl.when(has_right)
    def _():
        for c in halo_r():
            c.start()

    own_cp = [
        remote(own_pk.at[1 - gx], own_rx.at[gx, gz], own_sem.at[0, 0, 0], own_sem.at[1, gx, gz], (gz, 1 - gx, gy)),
        remote(own_pk.at[0], own_rx.at[gx, gz], own_sem.at[0, 0, 1], own_sem.at[1, gx, gz], (1 - gz, 0, gy)),
        remote(own_pk.at[1], own_rx.at[gx, gz], own_sem.at[0, 1, 0], own_sem.at[1, gx, gz], (1 - gz, 1, gy)),
    ]
    for c in own_cp:
        c.start()

    with jax.named_scope("wait_raw"):
        for c in raw_cp:
            c.wait()
    with jax.named_scope("fac1"):
        main_factors(1 - gx)
    g_cp = remote(gtx, grx, g_sem.at[0], g_sem.at[1], (1 - gz, gx, gy))
    g_cp.start()

    def forward_main(k):
        def block(b, totals):
            totals = list(totals)
            for i in range(16):
                z = zof(b * 16 + i)
                us = [raw[U, 0, z], raw[U, 1, z]]
                down = [roll(u, 1, 0) for u in us]
                up = [roll(u, 7, 0) for u in us]
                low = [jnp.where(row == 0, 0.0, down[0]), jnp.where(row == 0, down[0], down[1])]
                high = [jnp.where(row == 7, up[1], up[0]), jnp.where(row == 7, 0.0, up[1])]
                for t in range(2):
                    beside = (low[t] + high[t]) + (roll(us[t], 1) + roll(us[t], 127))
                    e = inv[k] * us[t] + raw[PC, t, z] * (beside - 4.0 * us[t]) + raw[SRC, t, z]
                    totals[t] = totals[t] + fac[k, t, z] * e
                    dsc[t, z] = totals[t]
            return tuple(totals)

        totals = lax.fori_loop(0, NJ // 16, block, (zero, zero))
        for t in range(2):
            dtx[k, t] = totals[t] * mid[0, k, t]
        cp = remote(dtx.at[k], drx.at[k], d_sem.at[0, k], d_sem.at[1, k], (1 - gz, gx, gy))
        cp.start()
        return cp

    def backward_main(k):
        last = zof(NJ - 1)
        ys = []
        for t in range(2):
            y = (dtx[k, t] + (1.0 - gtx[k, t]) * drx[k, t]) * mid[1, k, t]
            raw[U, t, last] = prv[k, t, last] * y
            ys.append(y)

        def block(b, ys):
            ys = list(ys)
            for i in range(7):
                z = zof(NJ - 2 - (b * 7 + i))
                for t in range(2):
                    ys[t] = ys[t] + dsc[t, z] * quo[k, t, z]
                    raw[U, t, z] = prv[k, t, z] * ys[t]
            return tuple(ys)

        lax.fori_loop(0, 9, block, tuple(ys))

    quads = [(x, z) for x in range(2) for z in range(2)]
    fills = {U: 0.0, PC: 0.0, SRC: 0.0, LC: LC_FILL}

    def unpack_own():
        def block(g, _):
            for jj in range(16):
                masks = [((lane - (64 * x + 32 * z + 4 + octet(jj))) & 127) < 8 for x, z in quads]
                for a in range(4):
                    v = jnp.full((8, 128), fills[a], jnp.float32)
                    for (x, z), m in zip(quads, masks):
                        v = jnp.where(m, own_rx[x, z, a, g], v)
                    est[a, g * 16 + jj] = roll(v, (-octet(jj)) % 128) if jj else v
            return 0

        lax.fori_loop(0, 4, block, 0)

    def unpack_halo():
        shifted = lane - 12 * gx

        def block(g, _):
            for jj in range(32):
                at = octet(jj) if jj < 16 else octet(jj - 16) + 4
                masks = [((shifted - (64 * x + 32 * z + at)) & 127) < 4 for x, z in quads]
                m_all = (shifted & 31) < 4
                for a in range(4):
                    v = zero
                    for (x, z), m in zip(quads, masks):
                        v = jnp.where(m, halo_rx[x, z, a, g], v)
                    v = roll(v, (-at) % 128) if at else v
                    est[a, g * 32 + jj] = jnp.where(m_all, v, est[a, g * 32 + jj])
            return 0

        lax.fori_loop(0, 2, block, 0)

    def edge_factors():
        def store(k, j, f, p, q):
            efac[k, j] = f
            eprv[k, j] = p
            equo[k, j] = q

        return factors(lambda j: est[LC, j], store)

    def other_half(v):
        return jnp.where((lane & 32) == 0, roll(v, 96), roll(v, 32))

    def edge_step(k, delta, recip):
        outer_low = (row == 0) & (lane < 64)
        outer_high = (row == 7) & (lane >= 64)

        def fwd(b, total):
            for i in range(16):
                j = b * 16 + i
                u = est[U, j]
                cross = roll(u, 64)
                low = jnp.where(outer_low, 0.0, roll(jnp.where(row == 7, cross, u), 1, 0))
                high = jnp.where(outer_high, 0.0, roll(jnp.where(row == 0, cross, u), 7, 0))
                beside = (low + high) + (roll(u, 1) + roll(u, 127))
                e = inv[k] * u + est[PC, j] * (beside - 4.0 * u) + est[SRC, j]
                total = total + efac[k, j] * e
                eds[j] = total
            return total

        total = lax.fori_loop(0, NJ // 16, fwd, zero)
        d = total * recip
        g = delta * recip
        last_p = eprv[k, NJ - 1]
        y = (d + (1.0 - g) * other_half(d)) / ((g + other_half(g) * (1.0 - g)) * last_p)
        est[U, NJ - 1] = last_p * y

        def back(b, y):
            for i in range(7):
                j = NJ - 2 - (b * 7 + i)
                y = y + eds[j] * equo[k, j]
                est[U, j] = eprv[k, j] * y
            return y

        lax.fori_loop(0, 9, back, y)

    with jax.named_scope("f0"):
        cp = forward_main(0)
    for c in own_cp:
        c.wait_send()
    for x, z in quads:

        @pl.when((x != gx) | (z != gz))
        def _():
            remote(own_rx.at[x, z], own_rx.at[x, z], own_sem.at[0, 0, 0], own_sem.at[1, x, z], (gz, 1 - gx, gy)).wait_recv()

    with jax.named_scope("unpack_own"):
        unpack_own()
    with jax.named_scope("wait_g"):
        g_cp.wait()
    for k in range(HALF):
        for t in range(2):
            g = gtx[k, t]
            mid[1, k, t] = 1.0 / ((g + grx[k, t] * (1.0 - g)) * prv[k, t, zof(NJ - 1)])
    with jax.named_scope("w0"):
        cp.wait()
    with jax.named_scope("b0"):
        backward_main(0)
    with jax.named_scope("f1"):
        cp = forward_main(1)
    with jax.named_scope("w1"):
        cp.wait()
    with jax.named_scope("b1"):
        backward_main(1)
    with jax.named_scope("f2"):
        cp = forward_main(2)

    @pl.when(has_left)
    def _():
        for c in halo_l():
            c.wait_send()

    @pl.when(has_right)
    def _():
        for c in halo_r():
            c.wait_send()

    @pl.when(((gx == 0) & has_left) | ((gx == 1) & has_right))
    def _():
        for x, z in quads:
            remote(halo_rx.at[x, z], halo_rx.at[x, z], halo_sem.at[0, 0, 0], halo_sem.at[1, x, z], (gz, 1 - gx, gy)).wait_recv()
        with jax.named_scope("unpack_halo"):
            unpack_halo()

    with jax.named_scope("edge_fac"):
        e_ps, e_ds, e_rs = edge_factors()
    with jax.named_scope("w2"):
        cp.wait()
    with jax.named_scope("b2"):
        backward_main(2)
    with jax.named_scope("f3"):
        cp = forward_main(3)
    for k in range(HALF):
        with jax.named_scope(f"e{k}"):
            edge_step(k, e_ds[k], e_rs[k])
    e_cp = remote(est.at[U], erx, e_sem.at[0], e_sem.at[1], (gz, 1 - gx, gy))
    e_cp.start()
    with jax.named_scope("w3"):
        cp.wait()
    with jax.named_scope("b3"):
        backward_main(3)
    with jax.named_scope("we"):
        e_cp.wait()

    def shift_of(side):
        return (120 * side - (base + 4 + 4 * side) + 4 * side + 256) % 128

    mine, other = shift_of(gx), shift_of(1 - gx)
    first, last = lane < 4, lane >= 124
    mine_mask = (first & (gx == 0)) | (last & (gx == 1))
    other_mask = (first & (gx == 1)) | (last & (gx == 0))

    def merge(b, _):
        for i in range(8):
            j = b * 8 + i
            z = zof(j)
            v = jnp.where(mine_mask, roll(est[U, j], mine), raw[U, gx, z])
            out_ref[z] = jnp.where(other_mask, roll(erx[j], other), v)
        return 0

    with jax.named_scope("merge"):
        lax.fori_loop(0, NJ // 8, merge, 0)


def solution(mesh):
    ny = mesh.shape["gy"]
    block = (NJ, 8, 128)
    vmem = lambda *s: pltpu.VMEM((*s, 8, 128), jnp.float32)

    def on_device(u, pc, lc, src, table, rows):
        hbm = pl.BlockSpec(memory_space=pl.ANY)
        smem = pl.BlockSpec(memory_space=pltpu.SMEM)
        return pl.pallas_call(
            functools.partial(kernel, ny),
            out_shape=jax.ShapeDtypeStruct(block, jnp.float32),
            in_specs=[hbm, hbm, hbm, hbm, smem, smem],
            out_specs=pl.BlockSpec(memory_space=pltpu.VMEM),
            scratch_shapes=[
                vmem(4, 2, NJ),
                vmem(HALF, 2, NJ), vmem(HALF, 2, NJ), vmem(HALF, 2, NJ),
                vmem(2, NJ), vmem(2, HALF, 2),
                vmem(HALF, 2), vmem(HALF, 2), vmem(HALF, 2), vmem(HALF, 2),
                vmem(2, 4, 4), vmem(2, 2, 4, 4), vmem(2, 4, 2), vmem(2, 2, 4, 2),
                vmem(4, NJ), vmem(HALF, NJ), vmem(HALF, NJ), vmem(HALF, NJ),
                vmem(NJ), vmem(NJ),
                pltpu.SemaphoreType.DMA((4,)),
                pltpu.SemaphoreType.DMA((2, 4)),
                pltpu.SemaphoreType.DMA((2, 2, 2)),
                pltpu.SemaphoreType.DMA((2, 2, 2)),
                pltpu.SemaphoreType.DMA((2,)),
                pltpu.SemaphoreType.DMA((2, HALF)),
                pltpu.SemaphoreType.DMA((2,)),
            ],
            compiler_params=pltpu.CompilerParams(collective_id=0, has_side_effects=True),
        )(u, pc, lc, src, table, rows)

    split = P("gz", "gx", "gy")
    return jax.shard_map(
        on_device, mesh=mesh, in_specs=(split,) * 4 + (P(), P()), out_specs=split, check_vma=False
    )
```

```python
import functools

import jax
import jax.numpy as jnp
from jax import lax
from jax.experimental import pallas as pl
from jax.experimental.pallas import tpu as pltpu
from jax.sharding import PartitionSpec as P

HALF = 4
NJ = 64
MESH = pl.DeviceIdType.MESH
U, PC, SRC, LC = range(4)
LC_FILL = 4000.0


def kernel(
    ny,
    u_hbm, pc_hbm, lc_hbm, src_hbm, table_hbm, rows_hbm,
    out_ref,
    raw, fac, prv, quo, dsc, mid, gtx, grx, dtx, drx,
    own_pk, own_rx, halo_pk, halo_rx, est, efac, eprv, equo, eds, erx,
    table, rows, load_sem, raw_sem, own_sem, halo_sem, g_sem, d0_sem, d_sem, e_sem, go,
):
    gz, gx, gy = lax.axis_index("gz"), lax.axis_index("gx"), lax.axis_index("gy")
    has_left, has_right = gy > 0, gy < ny - 1
    y_left, y_right = lax.rem(gy + ny - 1, ny), lax.rem(gy + 1, ny)
    lane = lax.broadcasted_iota(jnp.int32, (8, 128), 1)
    row = lax.broadcasted_iota(jnp.int32, (8, 128), 0)
    base = 64 * gx + 32 * gz
    ones = jnp.full((8, 128), 1.0, jnp.float32)
    zero = jnp.zeros((8, 128), jnp.float32)

    def zof(j):
        return jnp.where(gz == 0, j, NJ - 1 - j)

    def remote(src, dst, send, recv, dev):
        return pltpu.make_async_remote_copy(
            src_ref=src, dst_ref=dst, send_sem=send, recv_sem=recv, device_id=dev, device_id_type=MESH
        )

    def roll(v, amount, axis=1):
        return pltpu.roll(v, amount, axis)

    loads = [
        pltpu.make_async_copy(ref, raw.at[a, gx], load_sem.at[a])
        for a, ref in ((LC, lc_hbm), (U, u_hbm), (PC, pc_hbm), (SRC, src_hbm))
    ]
    loads.append(pltpu.make_async_copy(table_hbm, table, load_sem.at[4]))
    loads.append(pltpu.make_async_copy(rows_hbm, rows, load_sem.at[5]))
    for c in loads:
        c.start()
    barrier = pltpu.get_barrier_semaphore()

    def hello(sem, dev):
        pl.semaphore_signal(sem, inc=1, device_id=dev, device_id_type=MESH)

    hello(barrier, (1 - gz, 1, gy))

    @pl.when(gx == 0)
    def _():
        hello(barrier, (gz, 1, gy))

        @pl.when(has_left)
        def _():
            for z in range(2):
                hello(barrier, (z, 0, y_left))

    @pl.when((gx == 1) & has_right)
    def _():
        for z in range(2):
            hello(barrier, (z, 0, y_right))

    for c in loads:
        c.wait()

    low_half, even = (lane & 7) < 4, (lane & 8) == 0

    def pack(g, _):
        for a in range(4):
            left, right = [], []
            for h in range(2):
                both = []
                for q in range(2):
                    v = zero
                    for b in range(8):
                        at = 16 * b
                        w = roll(raw[a, gx, zof(g * 32 + h * 16 + q * 8 + b)], (at + 8) % 128)
                        v = w if b == 0 else jnp.where((lane >= at) & (lane < at + 16), w, v)
                    both.append(v)
                left.append(jnp.where(even, roll(both[0], 120), both[1]))
                right.append(jnp.where(even, both[0], roll(both[1], 8)))
            for h in range(2):
                own_pk[0, a, 2 * g + h] = roll(left[h], base + 4)
                own_pk[1, a, 2 * g + h] = roll(right[h], base + 4)
            halo_pk[0, a, g] = roll(jnp.where(low_half, left[0], roll(left[1], 4)), base + 12)
            halo_pk[1, a, g] = roll(jnp.where(low_half, roll(right[0], 124), right[1]), base)
        return 0

    def octet(jj):
        return 8 * (2 * jj if jj < 8 else 2 * (jj - 8) + 1)

    with jax.named_scope("pack"):
        lax.fori_loop(0, 2, pack, 0)
    for a in range(4):
        for g in range(4):
            own_rx[gx, gz, a, g] = own_pk[gx, a, g]

    inv = []
    for k in range(HALF):
        shift = jnp.float32(0.0)
        for i in range(table.shape[0]):
            shift = shift + jnp.where(rows[k] == i, table[i], 0.0)
        inv.append(1.0 / jnp.full((8, 128), shift, jnp.float32))

    def factors(load_lc, store):
        def block(b, carry):
            ps, ds, rs = carry
            ps, ds, rs = list(ps), list(ds), list(rs)
            for i in range(4):
                j = b * 4 + i
                t_line = 1.0 / load_lc(j)
                for k in range(HALF):
                    old, r_old = ps[k], rs[k]
                    ds[k] = ds[k] + (t_line * inv[k]) * old
                    ps[k] = old + ds[k]
                    rs[k] = 1.0 / ps[k]
                    store(k, j, t_line * old, old, r_old * rs[k])
            return tuple(ps), tuple(ds), tuple(rs)

        start = (ones,) * HALF
        return lax.fori_loop(0, NJ // 4, block, (start, start, start))

    def main_factors(t):
        def store(k, j, f, p, q):
            z = zof(j)
            fac[k, t, z] = f
            prv[k, t, z] = p
            quo[k, t, z] = q

        ps, ds, rs = factors(lambda j: raw[LC, t, zof(j)], store)
        for k in range(HALF):
            mid[0, k, t] = rs[k]
            gtx[t, k] = ds[k] * rs[k]

    with jax.named_scope("fac0"):
        main_factors(gx)

    with jax.named_scope("wait_barrier"):

        @pl.when(gx == 1)
        def _():
            pl.semaphore_wait(barrier, 3)
            hello(go, (gz, 0, gy))

        @pl.when(gx == 0)
        def _():
            pl.semaphore_wait(go, 1)

    raw_cp = {
        a: remote(raw.at[a, gx], raw.at[a, gx], raw_sem.at[0, a], raw_sem.at[1, a], (gz, 1 - gx, gy))
        for a in (U, LC, PC, SRC)
    }
    for c in raw_cp.values():
        c.start()

    def g_copy(x):
        return remote(gtx.at[gx], grx.at[gx], g_sem.at[0, x], g_sem.at[1, gx], (1 - gz, x, gy))

    for x in (1, 0):
        g_copy(x).start()

    def halo_l():
        return [
            remote(halo_pk.at[0], halo_rx.at[gx, gz], halo_sem.at[0, 0, z], halo_sem.at[1, gx, gz], (z, 1, y_left))
            for z in range(2)
        ]

    def halo_r():
        return [
            remote(halo_pk.at[1], halo_rx.at[gx, gz], halo_sem.at[0, 1, z], halo_sem.at[1, gx, gz], (z, 0, y_right))
            for z in range(2)
        ]

    own_cp = [
        remote(own_pk.at[1 - gx], own_rx.at[gx, gz], own_sem.at[0, 0, 0], own_sem.at[1, gx, gz], (gz, 1 - gx, gy)),
        remote(own_pk.at[0], own_rx.at[gx, gz], own_sem.at[0, 0, 1], own_sem.at[1, gx, gz], (1 - gz, 0, gy)),
        remote(own_pk.at[1], own_rx.at[gx, gz], own_sem.at[0, 1, 0], own_sem.at[1, gx, gz], (1 - gz, 1, gy)),
    ]

    def start_halos():
        @pl.when(gx == 0)
        def _():
            pl.semaphore_wait(barrier, 2 * has_left.astype(jnp.int32) + 2 * has_right.astype(jnp.int32))
            hello(go, (gz, 1, gy))

        @pl.when(gx == 1)
        def _():
            pl.semaphore_wait(go, 1)

        @pl.when(has_left)
        def _():
            for c in halo_l():
                c.start()

        @pl.when(has_right)
        def _():
            for c in halo_r():
                c.start()

    def d0_copy(x):
        return remote(dtx.at[0, gx], drx.at[0, gx], d0_sem.at[0, x], d0_sem.at[1, gx], (1 - gz, x, gy))

    def d_copy(k, x):
        return remote(dtx.at[k], drx.at[k], d_sem.at[x, k], d_sem.at[2, k], (1 - gz, x, gy))

    def wait_d(k):
        d_copy(k, 0).wait_recv()

    low_on, high_on = gx.astype(jnp.float32), (1 - gx).astype(jnp.float32)

    def forward_tile(t, low_on, high_on):
        def block(b, total):
            for i in range(32):
                z = zof(b * 32 + i)
                u, v = raw[U, t, z], raw[U, 1 - t, z]
                low = jnp.where(row == 0, roll(v, 1, 0) * low_on, roll(u, 1, 0))
                high = jnp.where(row == 7, roll(v, 7, 0) * high_on, roll(u, 7, 0))
                beside = (low + high) + (roll(u, 1) + roll(u, 127))
                e = inv[0] * u + raw[PC, t, z] * (beside - 4.0 * u) + raw[SRC, t, z]
                total = total + fac[0, t, z] * e
                dsc[t, z] = total
            return total

        dtx[0, t] = lax.fori_loop(0, NJ // 32, block, zero) * mid[0, 0, t]

    def forward_main(k):
        def block(b, totals):
            totals = list(totals)
            for i in range(32):
                z = zof(b * 32 + i)
                us = [raw[U, 0, z], raw[U, 1, z]]
                down = [roll(u, 1, 0) for u in us]
                up = [roll(u, 7, 0) for u in us]
                low = [jnp.where(row == 0, 0.0, down[0]), jnp.where(row == 0, down[0], down[1])]
                high = [jnp.where(row == 7, up[1], up[0]), jnp.where(row == 7, 0.0, up[1])]
                for t in range(2):
                    beside = (low[t] + high[t]) + (roll(us[t], 1) + roll(us[t], 127))
                    e = inv[k] * us[t] + raw[PC, t, z] * (beside - 4.0 * us[t]) + raw[SRC, t, z]
                    totals[t] = totals[t] + fac[k, t, z] * e
                    dsc[t, z] = totals[t]
            return tuple(totals)

        totals = lax.fori_loop(0, NJ // 32, block, (zero, zero))
        for t in range(2):
            dtx[k, t] = totals[t] * mid[0, k, t]
        @pl.when(gx == 1)
        def _():
            for x in (1, 0):
                d_copy(k, x).start()

    def backward_main(k):
        last = zof(NJ - 1)
        ys = []
        for t in range(2):
            y = (dtx[k, t] + (1.0 - gtx[t, k]) * drx[k, t]) * mid[1, k, t]
            raw[U, t, last] = prv[k, t, last] * y
            ys.append(y)

        def block(b, ys):
            ys = list(ys)
            for i in range(21):
                z = zof(NJ - 2 - (b * 21 + i))
                for t in range(2):
                    ys[t] = ys[t] + dsc[t, z] * quo[k, t, z]
                    raw[U, t, z] = prv[k, t, z] * ys[t]
            return tuple(ys)

        lax.fori_loop(0, 3, block, tuple(ys))

    quads = [(x, z) for x in range(2) for z in range(2)]
    fills = {U: 0.0, PC: 0.0, SRC: 0.0, LC: LC_FILL}

    def unpack_own():
        def block(g, _):
            for jj in range(16):
                masks = [((lane - (64 * x + 32 * z + 4 + octet(jj))) & 127) < 8 for x, z in quads]
                for a in range(4):
                    v = jnp.full((8, 128), fills[a], jnp.float32)
                    for (x, z), m in zip(quads, masks):
                        v = jnp.where(m, own_rx[x, z, a, g], v)
                    est[a, g * 16 + jj] = roll(v, (-octet(jj)) % 128) if jj else v
            return 0

        lax.fori_loop(0, 4, block, 0)

    def unpack_halo():
        shifted = lane - 12 * gx

        def block(g, _):
            for jj in range(32):
                at = octet(jj) if jj < 16 else octet(jj - 16) + 4
                masks = [((shifted - (64 * x + 32 * z + at)) & 127) < 4 for x, z in quads]
                m_all = (shifted & 31) < 4
                for a in range(4):
                    v = zero
                    for (x, z), m in zip(quads, masks):
                        v = jnp.where(m, halo_rx[x, z, a, g], v)
                    v = roll(v, (-at) % 128) if at else v
                    est[a, g * 32 + jj] = jnp.where(m_all, v, est[a, g * 32 + jj])
            return 0

        lax.fori_loop(0, 2, block, 0)

    def edge_factors():
        def store(k, j, f, p, q):
            efac[k, j] = f
            eprv[k, j] = p
            equo[k, j] = q

        return factors(lambda j: est[LC, j], store)

    def other_half(v):
        return jnp.where((lane & 32) == 0, roll(v, 96), roll(v, 32))

    def edge_step(k, delta, recip):
        outer_low = (row == 0) & (lane < 64)
        outer_high = (row == 7) & (lane >= 64)

        def fwd(b, total):
            for i in range(32):
                j = b * 32 + i
                u = est[U, j]
                cross = roll(u, 64)
                low = jnp.where(outer_low, 0.0, roll(jnp.where(row == 7, cross, u), 1, 0))
                high = jnp.where(outer_high, 0.0, roll(jnp.where(row == 0, cross, u), 7, 0))
                beside = (low + high) + (roll(u, 1) + roll(u, 127))
                e = inv[k] * u + est[PC, j] * (beside - 4.0 * u) + est[SRC, j]
                total = total + efac[k, j] * e
                eds[j] = total
            return total

        total = lax.fori_loop(0, NJ // 32, fwd, zero)
        d = total * recip
        g = delta * recip
        last_p = eprv[k, NJ - 1]
        y = (d + (1.0 - g) * other_half(d)) / ((g + other_half(g) * (1.0 - g)) * last_p)
        est[U, NJ - 1] = last_p * y

        def back(b, y):
            for i in range(21):
                j = NJ - 2 - (b * 21 + i)
                y = y + eds[j] * equo[k, j]
                est[U, j] = eprv[k, j] * y
            return y

        lax.fori_loop(0, 3, back, y)

    with jax.named_scope("wait_y"):
        start_halos()
    for c in own_cp:
        c.start()

    with jax.named_scope("wait_u"):
        raw_cp[U].wait()
    with jax.named_scope("f0"):
        forward_tile(gx, low_on, high_on)
        for x in (1, 0):
            d0_copy(x).start()
    with jax.named_scope("wait_raw"):
        for a in (LC, PC, SRC):
            raw_cp[a].wait()
    with jax.named_scope("fac1"):
        main_factors(1 - gx)
    with jax.named_scope("f0b"):
        forward_tile(1 - gx, high_on, low_on)
    with jax.named_scope("wait_g"):
        for x in range(2):
            g_copy(x).wait_send()
        for t in range(2):
            remote(gtx.at[t], grx.at[t], g_sem.at[0, 0], g_sem.at[1, t], (1 - gz, 0, gy)).wait_recv()
    for k in range(HALF):
        for t in range(2):
            g = gtx[t, k]
            mid[1, k, t] = 1.0 / ((g + grx[t, k] * (1.0 - g)) * prv[k, t, zof(NJ - 1)])
    with jax.named_scope("w0"):
        for x in range(2):
            d0_copy(x).wait_send()
        for t in range(2):
            remote(dtx.at[0, t], drx.at[0, t], d0_sem.at[0, 0], d0_sem.at[1, t], (1 - gz, 0, gy)).wait_recv()
    with jax.named_scope("b0"):
        backward_main(0)
    with jax.named_scope("f1"):
        forward_main(1)
    with jax.named_scope("wait_own"):
        for c in own_cp:
            c.wait_send()
        for x, z in quads:

            @pl.when((x != gx) | (z != gz))
            def _():
                remote(own_rx.at[x, z], own_rx.at[x, z], own_sem.at[0, 0, 0], own_sem.at[1, x, z], (gz, 1 - gx, gy)).wait_recv()

    with jax.named_scope("unpack_own"):
        unpack_own()
    @pl.when(has_left)
    def _():
        for c in halo_l():
            c.wait_send()

    @pl.when(has_right)
    def _():
        for c in halo_r():
            c.wait_send()

    @pl.when(((gx == 0) & has_left) | ((gx == 1) & has_right))
    def _():
      with jax.named_scope("wait_halo"):
        for x, z in quads:
            remote(halo_rx.at[x, z], halo_rx.at[x, z], halo_sem.at[0, 0, 0], halo_sem.at[1, x, z], (gz, 1 - gx, gy)).wait_recv()
        with jax.named_scope("unpack_halo"):
            unpack_halo()

    with jax.named_scope("edge_fac"):
        e_ps, e_ds, e_rs = edge_factors()
    with jax.named_scope("w1"):
        wait_d(1)
    with jax.named_scope("b1"):
        backward_main(1)
    with jax.named_scope("f2"):
        forward_main(2)

    for k in range(3):
        with jax.named_scope(f"e{k}"):
            edge_step(k, e_ds[k], e_rs[k])
    with jax.named_scope("w2"):
        wait_d(2)
    with jax.named_scope("b2"):
        backward_main(2)
    with jax.named_scope("f3"):
        forward_main(3)
    for k in range(3, HALF):
        with jax.named_scope(f"e{k}"):
            edge_step(k, e_ds[k], e_rs[k])
    e_cp = remote(est.at[U], erx, e_sem.at[0], e_sem.at[1], (gz, 1 - gx, gy))
    e_cp.start()
    with jax.named_scope("w3"):
        wait_d(3)
    with jax.named_scope("b3"):
        backward_main(3)
    with jax.named_scope("we"):
        e_cp.wait()

    @pl.when(gx == 1)
    def _():
        for k in range(1, HALF):
            for x in range(2):
                d_copy(k, x).wait_send()

    def shift_of(side):
        return (120 * side - (base + 4 + 4 * side) + 4 * side + 256) % 128

    mine, other = shift_of(gx), shift_of(1 - gx)
    first, last = lane < 4, lane >= 124
    mine_mask = (first & (gx == 0)) | (last & (gx == 1))
    other_mask = (first & (gx == 1)) | (last & (gx == 0))

    def merge(b, _):
        for i in range(32):
            j = b * 32 + i
            z = zof(j)
            v = jnp.where(mine_mask, roll(est[U, j], mine), raw[U, gx, z])
            out_ref[z] = jnp.where(other_mask, roll(erx[j], other), v)
        return 0

    with jax.named_scope("merge"):
        lax.fori_loop(0, NJ // 32, merge, 0)


def solution(mesh):
    ny = mesh.shape["gy"]
    block = (NJ, 8, 128)
    vmem = lambda *s: pltpu.VMEM((*s, 8, 128), jnp.float32)

    def on_device(u, pc, lc, src, table, rows):
        hbm = pl.BlockSpec(memory_space=pltpu.HBM)
        args = [pltpu.with_memory_space_constraint(x, pltpu.HBM) for x in (u, pc, lc, src, table, rows)]
        return pl.pallas_call(
            functools.partial(kernel, ny),
            out_shape=jax.ShapeDtypeStruct(block, jnp.float32),
            in_specs=[hbm] * 6,
            out_specs=pl.BlockSpec(memory_space=pltpu.VMEM),
            scratch_shapes=[
                vmem(4, 2, NJ),
                vmem(HALF, 2, NJ), vmem(HALF, 2, NJ), vmem(HALF, 2, NJ),
                vmem(2, NJ), vmem(2, HALF, 2),
                vmem(2, HALF), vmem(2, HALF), vmem(HALF, 2), vmem(HALF, 2),
                vmem(2, 4, 4), vmem(2, 2, 4, 4), vmem(2, 4, 2), vmem(2, 2, 4, 2),
                vmem(4, NJ), vmem(HALF, NJ), vmem(HALF, NJ), vmem(HALF, NJ),
                vmem(NJ), vmem(NJ),
                pltpu.SMEM((8,), jnp.float32), pltpu.SMEM((HALF,), jnp.int32),
                pltpu.SemaphoreType.DMA((6,)),
                pltpu.SemaphoreType.DMA((2, 4)),
                pltpu.SemaphoreType.DMA((2, 2, 2)),
                pltpu.SemaphoreType.DMA((2, 2, 2)),
                pltpu.SemaphoreType.DMA((2, 2)),
                pltpu.SemaphoreType.DMA((2, 2)),
                pltpu.SemaphoreType.DMA((3, HALF)),
                pltpu.SemaphoreType.DMA((2,)),
                pltpu.SemaphoreType.REGULAR,
            ],
            compiler_params=pltpu.CompilerParams(collective_id=0, has_side_effects=True, vmem_limit_bytes=24 * 2**20),
        )(*args)

    split = P("gz", "gx", "gy")
    return jax.shard_map(
        on_device, mesh=mesh, in_specs=(split,) * 4 + (P(), P()), out_specs=split, check_vma=False
    )
```

```python
import functools

import jax
import jax.numpy as jnp
from jax import lax
from jax.experimental import pallas as pl
from jax.experimental.pallas import tpu as pltpu
from jax.sharding import PartitionSpec as P

HALF = 4
NJ = 64
MESH = pl.DeviceIdType.MESH
U, PC, SRC, LC = range(4)
LC_FILL = 4000.0


def kernel(
    ny,
    u_hbm, pc_hbm, lc_hbm, src_hbm, table_hbm, rows_hbm,
    out_ref,
    raw, fac, prv, quo, dsc, mid, gtx, grx, dtx, drx,
    own_pk, own_rx, halo_pk, halo_rx, est, efac, eprv, equo, eds, emid, res_tx, res_rx, pass_rx, fin, fin_rx,
    table, rows, load_sem, raw_sem, own_sem, halo_sem, pass_sem, g_sem, d_sem, last_sem, fin_sem, e_sem, go,
):
    gz, gx, gy = lax.axis_index("gz"), lax.axis_index("gx"), lax.axis_index("gy")
    has_left, has_right = gy > 0, gy < ny - 1
    y_left, y_right = lax.rem(gy + ny - 1, ny), lax.rem(gy + 1, ny)
    lane = lax.broadcasted_iota(jnp.int32, (8, 128), 1)
    row = lax.broadcasted_iota(jnp.int32, (8, 128), 0)
    base = 64 * gx + 32 * gz
    ones = jnp.full((8, 128), 1.0, jnp.float32)
    zero = jnp.zeros((8, 128), jnp.float32)

    def zof(j):
        return jnp.where(gz == 0, j, NJ - 1 - j)

    def remote(src, dst, send, recv, dev):
        return pltpu.make_async_remote_copy(
            src_ref=src, dst_ref=dst, send_sem=send, recv_sem=recv, device_id=dev, device_id_type=MESH
        )

    def roll(v, amount, axis=1):
        return pltpu.roll(v, amount, axis)

    loads = [
        pltpu.make_async_copy(ref, raw.at[a, gx], load_sem.at[a])
        for a, ref in ((LC, lc_hbm), (U, u_hbm), (PC, pc_hbm), (SRC, src_hbm))
    ]
    loads.append(pltpu.make_async_copy(table_hbm, table, load_sem.at[4]))
    loads.append(pltpu.make_async_copy(rows_hbm, rows, load_sem.at[5]))
    for c in loads:
        c.start()
    barrier = pltpu.get_barrier_semaphore()

    def hello(sem, dev):
        pl.semaphore_signal(sem, inc=1, device_id=dev, device_id_type=MESH)

    hello(barrier, (1 - gz, 1, gy))

    @pl.when(gx == 0)
    def _():
        hello(barrier, (gz, 1, gy))

    @pl.when((gx == 0) & (gz == 0) & has_left)
    def _():
        for z in range(2):
            hello(barrier, (z, 0, y_left))

    @pl.when((gx == 0) & (gz == 1) & has_right)
    def _():
        for z in range(2):
            hello(barrier, (z, 0, y_right))

    for c in loads:
        c.wait()

    low_half, even = (lane & 7) < 4, (lane & 8) == 0

    def pack(g, _):
        for a in range(4):
            left, right = [], []
            for h in range(2):
                both = []
                for q in range(2):
                    v = zero
                    for b in range(8):
                        at = 16 * b
                        w = roll(raw[a, gx, zof(g * 32 + h * 16 + q * 8 + b)], (at + 8) % 128)
                        v = w if b == 0 else jnp.where((lane >= at) & (lane < at + 16), w, v)
                    both.append(v)
                left.append(jnp.where(even, roll(both[0], 120), both[1]))
                right.append(jnp.where(even, both[0], roll(both[1], 8)))
            for h in range(2):
                own_pk[0, a, 2 * g + h] = roll(left[h], base + 4)
                own_pk[1, a, 2 * g + h] = roll(right[h], base + 4)
            halo_pk[0, a, g] = roll(jnp.where(low_half, left[0], roll(left[1], 4)), base + 12)
            halo_pk[1, a, g] = roll(jnp.where(low_half, roll(right[0], 124), right[1]), base)
        return 0

    def octet(jj):
        return 8 * (2 * jj if jj < 8 else 2 * (jj - 8) + 1)

    with jax.named_scope("pack"):
        lax.fori_loop(0, 2, pack, 0)

    with jax.named_scope("wait_barrier"):

        @pl.when(gx == 1)
        def _():
            pl.semaphore_wait(barrier, 3)
            hello(go, (gz, 0, gy))

        @pl.when(gx == 0)
        def _():
            pl.semaphore_wait(go, 1)

    raw_cp = {
        a: remote(raw.at[a, 0], raw.at[a, 0], raw_sem.at[0, a], raw_sem.at[1, a], (gz, 1, gy)) for a in (LC, U, PC, SRC)
    }
    pass_cp = remote(halo_pk, pass_rx, pass_sem.at[0], pass_sem.at[1], (gz, 0, gy))

    def halo_copies(side, dev):
        return [
            remote(pk.at[side], halo_rx.at[x, gz], halo_sem.at[0, side, x], halo_sem.at[1, x, gz], dev)
            for x, pk in ((0, halo_pk), (1, pass_rx))
        ]

    def halo_l():
        return halo_copies(0, (1, 0, y_left))

    def halo_r():
        return halo_copies(1, (0, 0, y_right))

    own_far = remote(own_pk.at[1 - gz], own_rx.at[gx, gz], own_sem.at[0, 0, 0], own_sem.at[1, gx, gz], (1 - gz, 0, gy))
    own_near = remote(own_pk.at[gz], own_rx.at[1, gz], own_sem.at[0, 0, 1], own_sem.at[1, 1, gz], (gz, 0, gy))
    g_cp = remote(gtx, grx, g_sem.at[0], g_sem.at[1], (1 - gz, 1, gy))

    def d_copy(k):
        return remote(dtx.at[k], drx.at[k], d_sem.at[0, k], d_sem.at[1, k], (1 - gz, 1, gy))

    def wait_d(k):
        d_copy(k).wait_recv()

    last_copy = remote(dtx.at[HALF - 1, 0], drx.at[HALF - 1, 0], last_sem.at[0], last_sem.at[1], (1 - gz, 0, gy))
    dsc_cp = remote(dsc.at[0], dsc.at[0], fin_sem.at[0, 0], fin_sem.at[1, 0], (gz, 0, gy))
    fin_cp = remote(fin, fin_rx, fin_sem.at[0, 1], fin_sem.at[1, 1], (gz, 0, gy))

    inv = []
    for k in range(HALF):
        shift = jnp.float32(0.0)
        for i in range(table.shape[0]):
            shift = shift + jnp.where(rows[k] == i, table[i], 0.0)
        inv.append(1.0 / jnp.full((8, 128), shift, jnp.float32))

    def factors(load_lc, store):
        def block(b, carry):
            ps, ds, rs = carry
            ps, ds, rs = list(ps), list(ds), list(rs)
            for i in range(16):
                j = b * 16 + i
                t_line = 1.0 / load_lc(j)
                for k in range(HALF):
                    old, r_old = ps[k], rs[k]
                    ds[k] = ds[k] + (t_line * inv[k]) * old
                    ps[k] = old + ds[k]
                    rs[k] = 1.0 / ps[k]
                    store(k, j, t_line * old, old, r_old * rs[k])
            return tuple(ps), tuple(ds), tuple(rs)

        start = (ones,) * HALF
        return lax.fori_loop(0, NJ // 16, block, (start, start, start))

    def main_factors(t):
        def store(k, j, f, p, q):
            z = zof(j)
            fac[k, t, z] = f
            prv[k, t, z] = p
            quo[k, t, z] = q

        ps, ds, rs = factors(lambda j: raw[LC, t, zof(j)], store)
        for k in range(HALF):
            mid[0, k, t] = rs[k]
            gtx[t, k] = ds[k] * rs[k]

    def forward_main(k):
        def block(b, totals):
            totals = list(totals)
            for i in range(32):
                z = zof(b * 32 + i)
                us = [raw[U, 0, z], raw[U, 1, z]]
                down = [roll(u, 1, 0) for u in us]
                up = [roll(u, 7, 0) for u in us]
                low = [jnp.where(row == 0, 0.0, down[0]), jnp.where(row == 0, down[0], down[1])]
                high = [jnp.where(row == 7, up[1], up[0]), jnp.where(row == 7, 0.0, up[1])]
                for t in range(2):
                    beside = (low[t] + high[t]) + (roll(us[t], 1) + roll(us[t], 127))
                    e = inv[k] * us[t] + raw[PC, t, z] * (beside - 4.0 * us[t]) + raw[SRC, t, z]
                    totals[t] = totals[t] + fac[k, t, z] * e
                    dsc[t, z] = totals[t]
            return tuple(totals)

        totals = lax.fori_loop(0, NJ // 32, block, (zero, zero))
        for t in range(2):
            dtx[k, t] = totals[t] * mid[0, k, t]
        d_copy(k).start()
        if k == HALF - 1:
            last_copy.start()

    def backward_main(k):
        last = zof(NJ - 1)
        ys = []
        for t in range(2):
            y = (dtx[k, t] + (1.0 - gtx[t, k]) * drx[k, t]) * mid[1, k, t]
            raw[U, t, last] = prv[k, t, last] * y
            ys.append(y)

        def block(b, ys):
            ys = list(ys)
            for i in range(21):
                z = zof(NJ - 2 - (b * 21 + i))
                for t in range(2):
                    ys[t] = ys[t] + dsc[t, z] * quo[k, t, z]
                    raw[U, t, z] = prv[k, t, z] * ys[t]
            return tuple(ys)

        lax.fori_loop(0, 3, block, tuple(ys))

    quads = [(x, z) for x in range(2) for z in range(2)]
    fills = {U: 0.0, PC: 0.0, SRC: 0.0, LC: LC_FILL}

    def unpack_own():
        def block(g, _):
            for jj in range(16):
                masks = [((lane - (64 * x + 32 * z + 4 + octet(jj))) & 127) < 8 for x, z in quads]
                for a in range(4):
                    v = jnp.full((8, 128), fills[a], jnp.float32)
                    for (x, z), m in zip(quads, masks):
                        v = jnp.where(m, own_rx[x, z, a, g], v)
                    est[a, g * 16 + jj] = roll(v, (-octet(jj)) % 128) if jj else v
            return 0

        lax.fori_loop(0, 4, block, 0)

    def unpack_halo():
        shifted = lane - 12 * gz

        def block(g, _):
            for jj in range(32):
                at = octet(jj) if jj < 16 else octet(jj - 16) + 4
                masks = [((shifted - (64 * x + 32 * z + at)) & 127) < 4 for x, z in quads]
                m_all = (shifted & 31) < 4
                for a in range(4):
                    v = zero
                    for (x, z), m in zip(quads, masks):
                        v = jnp.where(m, halo_rx[x, z, a, g], v)
                    v = roll(v, (-at) % 128) if at else v
                    est[a, g * 32 + jj] = jnp.where(m_all, v, est[a, g * 32 + jj])
            return 0

        lax.fori_loop(0, 2, block, 0)

    def edge_factors():
        def store(k, j, f, p, q):
            efac[k, j] = f
            eprv[k, j] = p
            equo[k, j] = q

        ps, ds, rs = factors(lambda j: est[LC, j], store)
        for k in range(HALF):
            emid[0, k] = ds[k] * rs[k]
            emid[1, k] = rs[k]

    def other_half(v):
        return jnp.where((lane & 32) == 0, roll(v, 96), roll(v, 32))

    def edge_step(k):
        outer_low = (row == 0) & (lane < 64)
        outer_high = (row == 7) & (lane >= 64)

        def fwd(b, total):
            for i in range(32):
                j = b * 32 + i
                u = est[U, j]
                cross = roll(u, 64)
                low = jnp.where(outer_low, 0.0, roll(jnp.where(row == 7, cross, u), 1, 0))
                high = jnp.where(outer_high, 0.0, roll(jnp.where(row == 0, cross, u), 7, 0))
                beside = (low + high) + (roll(u, 1) + roll(u, 127))
                e = inv[k] * u + est[PC, j] * (beside - 4.0 * u) + est[SRC, j]
                total = total + efac[k, j] * e
                eds[j] = total
            return total

        total = lax.fori_loop(0, NJ // 32, fwd, zero)
        d = total * emid[1, k]
        g = emid[0, k]
        last_p = eprv[k, NJ - 1]
        y = (d + (1.0 - g) * other_half(d)) / ((g + other_half(g) * (1.0 - g)) * last_p)
        est[U, NJ - 1] = last_p * y

        def back(b, y):
            for i in range(21):
                j = NJ - 2 - (b * 21 + i)
                y = y + eds[j] * equo[k, j]
                est[U, j] = eprv[k, j] * y
            return y

        lax.fori_loop(0, 3, back, y)

    def pack_result():
        shifted = lane - 4 * gz
        outs = [[zero, zero] for _ in quads]
        for i in range(32):
            us = [est[U, i], est[U, 32 + i]]
            if i:
                us = [roll(u, 4 * i) for u in us]
            for n, (x, z) in enumerate(quads):
                m = ((shifted - (64 * x + 32 * z + 4 + 4 * i)) & 127) < 4
                for h in range(2):
                    outs[n][h] = jnp.where(m, us[h], outs[n][h])
        for n, (x, z) in enumerate(quads):
            for h in range(2):
                res_tx[x, z, h] = roll(outs[n][h], lax.rem(120 * gz + 256 - (64 * x + 32 * z + 4), 128))
        for h in range(2):
            res_rx[gz, h] = res_tx[0, gz, h]

    def res_copy(x, z):
        return remote(res_tx.at[x, z], res_rx.at[gz], e_sem.at[x, z, 0], e_sem.at[2, gz, 0], (z, x, gy))

    def main_problem():
        pass_cp.start()
        own_near.start()
        with jax.named_scope("fac1"):
            main_factors(1)
        with jax.named_scope("wait_lc"):
            raw_cp[LC].wait_recv()
        with jax.named_scope("fac0m"):
            main_factors(0)
        g_cp.start()
        with jax.named_scope("wait_raw"):
            for a in (U, PC, SRC):
                raw_cp[a].wait_recv()
        with jax.named_scope("f0"):
            forward_main(0)
        own_far.start()
        with jax.named_scope("wait_g"):
            g_cp.wait()
        for k in range(HALF):
            for t in range(2):
                g = gtx[t, k]
                mid[1, k, t] = 1.0 / ((g + grx[t, k] * (1.0 - g)) * prv[k, t, zof(NJ - 1)])
        for k in range(1, HALF):
            with jax.named_scope(f"w{k - 1}"):
                wait_d(k - 1)
            with jax.named_scope(f"b{k - 1}"):
                backward_main(k - 1)
            with jax.named_scope(f"f{k}"):
                forward_main(k)
        dsc_cp.start()
        fin[0] = dtx[HALF - 1, 0] * mid[1, HALF - 1, 0]
        fin[1] = (1.0 - gtx[0, HALF - 1]) * mid[1, HALF - 1, 0]
        fin_cp.start()

    def edge_problem():
        for a in range(4):
            for g in range(4):
                own_rx[gx, gz, a, g] = own_pk[gz, a, g]
        with jax.named_scope("fac0"):
            main_factors(0)
        with jax.named_scope("wait_own"):
            for x, z in quads:

                @pl.when((x == 1) | (z != gz))
                def _():
                    remote(own_rx.at[x, z], own_rx.at[x, z], own_sem.at[0, 0, 0], own_sem.at[1, x, z], (gz, 1, gy)).wait_recv()

        with jax.named_scope("unpack_own"):
            unpack_own()

        @pl.when(((gz == 0) & has_left) | ((gz == 1) & has_right))
        def _():
            with jax.named_scope("wait_halo"):
                for x, z in quads:
                    remote(halo_rx.at[x, z], halo_rx.at[x, z], halo_sem.at[0, 0, 0], halo_sem.at[1, x, z], (gz, 1, gy)).wait_recv()
            with jax.named_scope("unpack_halo"):
                unpack_halo()

        with jax.named_scope("edge_fac"):
            edge_factors()
        for k in range(HALF):
            with jax.named_scope(f"e{k}"):
                edge_step(k)
        with jax.named_scope("epack"):
            pack_result()
        for x, z in ((1, 0), (1, 1), (0, 0), (0, 1)):

            @pl.when((x == 1) | (z != gz))
            def _():
                res_copy(x, z).start()

    @pl.when(gx == 1)
    def _():
        main_problem()

    @pl.when(gx == 0)
    def _():
        for c in raw_cp.values():
            c.start()
        with jax.named_scope("wait_pass"):
            pass_cp.wait_recv()
        with jax.named_scope("wait_y"):
            pl.semaphore_wait(barrier, has_left.astype(jnp.int32) + has_right.astype(jnp.int32))

        @pl.when(has_left)
        def _():
            for c in halo_l():
                c.start()

        @pl.when(has_right)
        def _():
            for c in halo_r():
                c.start()

        own_far.start()
        edge_problem()

    with jax.named_scope("we"):
        for side in range(2):

            @pl.when((gx == 1) | (gz != side))
            def _():
                remote(res_rx.at[side], res_rx.at[side], e_sem.at[0, 0, 0], e_sem.at[2, side, 0], (gz, 1 - gx, gy)).wait_recv()

    first, last = lane < 4, lane >= 124

    def finish(t, y):
        k = HALF - 1
        for j in reversed(range(NJ)):
            z, at = zof(j), (-4 * (j % 32)) % 128
            left, right = res_rx[0, j // 32], res_rx[1, j // 32]
            if at:
                left, right = roll(left, at), roll(right, at)
            if j < NJ - 1:
                y = y + dsc[t, z] * quo[k, t, z]
            out_ref[z] = jnp.where(last, right, jnp.where(first, left, prv[k, t, z] * y))

    @pl.when(gx == 1)
    def _():
        k = HALF - 1
        with jax.named_scope("w3"):
            wait_d(k)
        with jax.named_scope("finish"):
            finish(1, (dtx[k, 1] + (1.0 - gtx[1, k]) * drx[k, 1]) * mid[1, k, 1])
        pass_cp.wait_send()
        own_near.wait_send()
        for i in range(HALF):
            d_copy(i).wait_send()
        last_copy.wait_send()
        dsc_cp.wait_send()
        fin_cp.wait_send()

    @pl.when(gx == 0)
    def _():
        with jax.named_scope("w3s"):
            dsc_cp.wait_recv()
            fin_cp.wait_recv()
            last_copy.wait_recv()
        with jax.named_scope("finish_s"):
            finish(0, fin_rx[0] + fin_rx[1] * drx[HALF - 1, 0])
        for c in raw_cp.values():
            c.wait_send()
        for x, z in quads:

            @pl.when((x == 1) | (z != gz))
            def _():
                res_copy(x, z).wait_send()

        @pl.when(has_left)
        def _():
            for c in halo_l():
                c.wait_send()

        @pl.when(has_right)
        def _():
            for c in halo_r():
                c.wait_send()

    own_far.wait_send()


def solution(mesh):
    ny = mesh.shape["gy"]
    block = (NJ, 8, 128)
    vmem = lambda *s: pltpu.VMEM((*s, 8, 128), jnp.float32)

    def on_device(u, pc, lc, src, table, rows):
        hbm = pl.BlockSpec(memory_space=pltpu.HBM)
        args = [pltpu.with_memory_space_constraint(x, pltpu.HBM) for x in (u, pc, lc, src, table, rows)]
        return pl.pallas_call(
            functools.partial(kernel, ny),
            out_shape=jax.ShapeDtypeStruct(block, jnp.float32),
            in_specs=[hbm] * 6,
            out_specs=pl.BlockSpec(memory_space=pltpu.VMEM),
            scratch_shapes=[
                vmem(4, 2, NJ),
                vmem(HALF, 2, NJ), vmem(HALF, 2, NJ), vmem(HALF, 2, NJ),
                vmem(2, NJ), vmem(2, HALF, 2),
                vmem(2, HALF), vmem(2, HALF), vmem(HALF, 2), vmem(HALF, 2),
                vmem(2, 4, 4), vmem(2, 2, 4, 4), vmem(2, 4, 2), vmem(2, 2, 4, 2),
                vmem(4, NJ), vmem(HALF, NJ), vmem(HALF, NJ), vmem(HALF, NJ),
                vmem(NJ), vmem(2, HALF), vmem(2, 2, 2), vmem(2, 2), vmem(2, 4, 2), vmem(2), vmem(2),
                pltpu.SMEM((8,), jnp.float32), pltpu.SMEM((HALF,), jnp.int32),
                pltpu.SemaphoreType.DMA((6,)),
                pltpu.SemaphoreType.DMA((2, 4)),
                pltpu.SemaphoreType.DMA((2, 2, 2)),
                pltpu.SemaphoreType.DMA((2, 2, 2)),
                pltpu.SemaphoreType.DMA((2,)),
                pltpu.SemaphoreType.DMA((2,)),
                pltpu.SemaphoreType.DMA((2, HALF)),
                pltpu.SemaphoreType.DMA((2,)),
                pltpu.SemaphoreType.DMA((2, 2)),
                pltpu.SemaphoreType.DMA((3, 2, 1)),
                pltpu.SemaphoreType.REGULAR,
            ],
            compiler_params=pltpu.CompilerParams(collective_id=0, has_side_effects=True, vmem_limit_bytes=24 * 2**20),
        )(*args)

    split = P("gz", "gx", "gy")
    return jax.shard_map(
        on_device, mesh=mesh, in_specs=(split,) * 4 + (P(), P()), out_specs=split, check_vma=False
    )
```

```python
import functools

import jax
import jax.numpy as jnp
from jax import lax
from jax.experimental import pallas as pl
from jax.experimental.pallas import tpu as pltpu
from jax.sharding import PartitionSpec as P

HALF = 4
NJ = 64
MESH = pl.DeviceIdType.MESH
U, PC, SRC, LC = range(4)
LC_FILL = 4000.0


def kernel(
    ny,
    u_hbm, pc_hbm, lc_hbm, src_hbm, table_hbm, rows_hbm,
    out_ref,
    raw, fac, prv, quo, dsc, mid, gtx, grx, dtx, drx,
    own_pk, own_rx, halo_pk, halo_rx, est, efac, eprv, equo, eds, emid, res_tx, res_rx, pass_rx, fin, fin_rx,
    table, rows, load_sem, raw_sem, own_sem, halo_sem, pass_sem, g_sem, d_sem, last_sem, fin_sem, e_sem, go,
):
    gz, gx, gy = lax.axis_index("gz"), lax.axis_index("gx"), lax.axis_index("gy")
    has_left, has_right = gy > 0, gy < ny - 1
    y_left, y_right = lax.rem(gy + ny - 1, ny), lax.rem(gy + 1, ny)
    lane = lax.broadcasted_iota(jnp.int32, (8, 128), 1)
    row = lax.broadcasted_iota(jnp.int32, (8, 128), 0)
    base = 64 * gx + 32 * gz
    ones = jnp.full((8, 128), 1.0, jnp.float32)
    zero = jnp.zeros((8, 128), jnp.float32)

    def zof(j):
        return jnp.where(gz == 0, j, NJ - 1 - j)

    def remote(src, dst, send, recv, dev):
        return pltpu.make_async_remote_copy(
            src_ref=src, dst_ref=dst, send_sem=send, recv_sem=recv, device_id=dev, device_id_type=MESH
        )

    def roll(v, amount, axis=1):
        return pltpu.roll(v, amount, axis)

    loads = [
        pltpu.make_async_copy(ref, raw.at[a, gx], load_sem.at[a])
        for a, ref in ((LC, lc_hbm), (U, u_hbm), (PC, pc_hbm), (SRC, src_hbm))
    ]
    loads.append(pltpu.make_async_copy(table_hbm, table, load_sem.at[4]))
    loads.append(pltpu.make_async_copy(rows_hbm, rows, load_sem.at[5]))
    for c in loads:
        c.start()
    barrier = pltpu.get_barrier_semaphore()

    def hello(sem, dev):
        pl.semaphore_signal(sem, inc=1, device_id=dev, device_id_type=MESH)

    hello(barrier, (1 - gz, 1, gy))

    @pl.when(gx == 0)
    def _():
        hello(barrier, (gz, 1, gy))

    @pl.when((gx == 0) & (gz == 0) & has_left)
    def _():
        for z in range(2):
            hello(barrier, (z, 0, y_left))

    @pl.when((gx == 0) & (gz == 1) & has_right)
    def _():
        for z in range(2):
            hello(barrier, (z, 0, y_right))

    with jax.named_scope("wait_barrier"):

        @pl.when(gx == 1)
        def _():
            pl.semaphore_wait(barrier, 3)
            hello(go, (gz, 0, gy))

        @pl.when(gx == 0)
        def _():
            pl.semaphore_wait(go, 1)

    for c in loads:
        c.wait()

    raw_cp = {
        a: remote(raw.at[a, 0], raw.at[a, 0], raw_sem.at[0, a], raw_sem.at[1, a], (gz, 1, gy)) for a in (LC, U, PC, SRC)
    }

    @pl.when(gx == 0)
    def _():
        for c in raw_cp.values():
            c.start()


    spot = (lane - base - 4) & 127
    low_half, even = (spot & 7) < 4, (spot & 8) == 0
    group = jnp.where(gz == 0, spot >> 4, 7 - (spot >> 4))
    places = [(base + 12 + jnp.where(gz == 0, 16 * b, 112 - 16 * b)) & 127 for b in range(8)]
    forwards = jnp.full((8, 128), gz, jnp.int32) == 0

    def in_order(pair):
        return jnp.where(forwards, pair[0], pair[1]), jnp.where(forwards, pair[1], pair[0])

    def pack(g, _):
        at = jnp.where(gz == 0, g, 1 - g)
        for a in range(4):
            left, right = [], []
            for h in range(2):
                both = []
                for q in range(2):
                    v = zero
                    for b in range(8):
                        w = roll(raw[a, gx, g * 32 + (h * 16 + q * 8 + b)], places[b])
                        v = w if b == 0 else jnp.where(group == b, w, v)
                    both.append(v)
                both = in_order(both)
                left.append(jnp.where(even, roll(both[0], 120), both[1]))
                right.append(jnp.where(even, both[0], roll(both[1], 8)))
            left, right = in_order(left), in_order(right)
            for h in range(2):
                own_pk[0, a, 2 * at + h] = left[h]
                own_pk[1, a, 2 * at + h] = right[h]
            halo_pk[0, a, at] = jnp.where(low_half, roll(left[0], 8), roll(left[1], 12))
            halo_pk[1, a, at] = jnp.where(low_half, roll(right[1], 124), roll(right[0], 120))
        return 0

    def octet(jj):
        return 8 * (2 * jj if jj < 8 else 2 * (jj - 8) + 1)

    with jax.named_scope("pack"):
        lax.fori_loop(0, 2, pack, 0)

    pass_cp = remote(halo_pk, pass_rx, pass_sem.at[0], pass_sem.at[1], (gz, 0, gy))

    def halo_copy(x, side):
        pk, dev = (halo_pk, pass_rx)[x], ((1, 0, y_left), (0, 0, y_right))[side]
        return remote(pk.at[side], halo_rx.at[x, gz], halo_sem.at[0, side, x], halo_sem.at[1, x, gz], dev)

    own_far = remote(own_pk.at[1 - gz], own_rx.at[gx, gz], own_sem.at[0, 0, 0], own_sem.at[1, gx, gz], (1 - gz, 0, gy))
    own_near = remote(own_pk.at[gz], own_rx.at[1, gz], own_sem.at[0, 0, 1], own_sem.at[1, 1, gz], (gz, 0, gy))
    g_cp = remote(gtx, grx, g_sem.at[0], g_sem.at[1], (1 - gz, 1, gy))

    def d_copy(k):
        return remote(dtx.at[k], drx.at[k], d_sem.at[0, k], d_sem.at[1, k], (1 - gz, 1, gy))

    def wait_d(k):
        d_copy(k).wait_recv()

    last_copy = remote(dtx.at[HALF - 1, 0], drx.at[HALF - 1, 0], last_sem.at[0], last_sem.at[1], (1 - gz, 0, gy))
    dsc_cp = remote(dsc.at[0], dsc.at[0], fin_sem.at[0, 0], fin_sem.at[1, 0], (gz, 0, gy))
    fin_cp = remote(fin, fin_rx, fin_sem.at[0, 1], fin_sem.at[1, 1], (gz, 0, gy))

    inv = []
    for k in range(HALF):
        shift = jnp.float32(0.0)
        for i in range(table.shape[0]):
            shift = shift + jnp.where(rows[k] == i, table[i], 0.0)
        inv.append(1.0 / jnp.full((8, 128), shift, jnp.float32))

    def factors(load_lc, store):
        def block(b, carry):
            ps, ds, rs = carry
            ps, ds, rs = list(ps), list(ds), list(rs)
            for i in range(16):
                j = b * 16 + i
                t_line = 1.0 / load_lc(j)
                for k in range(HALF):
                    old, r_old = ps[k], rs[k]
                    ds[k] = ds[k] + (t_line * inv[k]) * old
                    ps[k] = old + ds[k]
                    rs[k] = 1.0 / ps[k]
                    store(k, j, t_line * old, old, r_old * rs[k])
            return tuple(ps), tuple(ds), tuple(rs)

        start = (ones,) * HALF
        return lax.fori_loop(0, NJ // 16, block, (start, start, start))

    def main_factors(t):
        def store(k, j, f, p, q):
            z = zof(j)
            fac[k, t, z] = f
            prv[k, t, z] = p
            quo[k, t, z] = q

        ps, ds, rs = factors(lambda j: raw[LC, t, zof(j)], store)
        for k in range(HALF):
            mid[0, k, t] = rs[k]
            gtx[t, k] = ds[k] * rs[k]

    def forward_main(k):
        def block(b, totals):
            totals = list(totals)
            for i in range(64):
                z = zof(i)
                us = [raw[U, 0, z], raw[U, 1, z]]
                down = [roll(u, 1, 0) for u in us]
                up = [roll(u, 7, 0) for u in us]
                low = [jnp.where(row == 0, 0.0, down[0]), jnp.where(row == 0, down[0], down[1])]
                high = [jnp.where(row == 7, up[1], up[0]), jnp.where(row == 7, 0.0, up[1])]
                for t in range(2):
                    beside = (low[t] + high[t]) + (roll(us[t], 1) + roll(us[t], 127))
                    e = inv[k] * us[t] + raw[PC, t, z] * (beside - 4.0 * us[t]) + raw[SRC, t, z]
                    totals[t] = totals[t] + fac[k, t, z] * e
                    dsc[t, z] = totals[t]
            return tuple(totals)

        totals = block(0, (zero, zero))
        for t in range(2):
            dtx[k, t] = totals[t] * mid[0, k, t]
        d_copy(k).start()
        if k == HALF - 1:
            last_copy.start()

    def backward_main(k):
        last = zof(NJ - 1)
        ys = []
        for t in range(2):
            y = (dtx[k, t] + (1.0 - gtx[t, k]) * drx[k, t]) * mid[1, k, t]
            raw[U, t, last] = prv[k, t, last] * y
            ys.append(y)

        def block(b, ys):
            ys = list(ys)
            for i in range(21):
                z = zof(NJ - 2 - (b * 21 + i))
                for t in range(2):
                    ys[t] = ys[t] + dsc[t, z] * quo[k, t, z]
                    raw[U, t, z] = prv[k, t, z] * ys[t]
            return tuple(ys)

        lax.fori_loop(0, 3, block, tuple(ys))

    quads = [(x, z) for x in range(2) for z in range(2)]
    fills = {U: 0.0, PC: 0.0, SRC: 0.0, LC: LC_FILL}

    def unpack_own():
        def block(g, _):
            for jj in range(16):
                masks = [((lane - (64 * x + 32 * z + 4 + octet(jj))) & 127) < 8 for x, z in quads]
                for a in range(4):
                    v = jnp.full((8, 128), fills[a], jnp.float32)
                    for (x, z), m in zip(quads, masks):
                        v = jnp.where(m, own_rx[x, z, a, g], v)
                    est[a, g * 16 + jj] = roll(v, (-octet(jj)) % 128) if jj else v
            return 0

        lax.fori_loop(0, 4, block, 0)

    def unpack_halo():
        shifted = lane - 12 * gz

        def block(g, _):
            for jj in range(32):
                at = octet(jj) if jj < 16 else octet(jj - 16) + 4
                masks = [((shifted - (64 * x + 32 * z + at)) & 127) < 4 for x, z in quads]
                m_all = (shifted & 31) < 4
                for a in range(4):
                    v = zero
                    for (x, z), m in zip(quads, masks):
                        v = jnp.where(m, halo_rx[x, z, a, g], v)
                    v = roll(v, (-at) % 128) if at else v
                    est[a, g * 32 + jj] = jnp.where(m_all, v, est[a, g * 32 + jj])
            return 0

        lax.fori_loop(0, 2, block, 0)

    def edge_factors():
        def store(k, j, f, p, q):
            efac[k, j] = f
            eprv[k, j] = p
            equo[k, j] = q

        ps, ds, rs = factors(lambda j: est[LC, j], store)
        for k in range(HALF):
            emid[0, k] = ds[k] * rs[k]
            emid[1, k] = rs[k]

    def other_half(v):
        return jnp.where((lane & 32) == 0, roll(v, 96), roll(v, 32))

    def edge_step(k):
        outer_low = (row == 0) & (lane < 64)
        outer_high = (row == 7) & (lane >= 64)

        def fwd(b, total):
            for i in range(64):
                j = i
                u = est[U, j]
                cross = roll(u, 64)
                low = jnp.where(outer_low, 0.0, roll(jnp.where(row == 7, cross, u), 1, 0))
                high = jnp.where(outer_high, 0.0, roll(jnp.where(row == 0, cross, u), 7, 0))
                beside = (low + high) + (roll(u, 1) + roll(u, 127))
                e = inv[k] * u + est[PC, j] * (beside - 4.0 * u) + est[SRC, j]
                total = total + efac[k, j] * e
                eds[j] = total
            return total

        total = fwd(0, zero)
        d = total * emid[1, k]
        g = emid[0, k]
        last_p = eprv[k, NJ - 1]
        y = (d + (1.0 - g) * other_half(d)) / ((g + other_half(g) * (1.0 - g)) * last_p)
        est[U, NJ - 1] = last_p * y

        for j in reversed(range(NJ - 1)):
            y = y + eds[j] * equo[k, j]
            est[U, j] = eprv[k, j] * y

    def pack_result():
        shifted = lane - 4 * gz
        outs = [[zero, zero] for _ in quads]
        for i in range(32):
            us = [est[U, i], est[U, 32 + i]]
            if i:
                us = [roll(u, 4 * i) for u in us]
            for n, (x, z) in enumerate(quads):
                m = ((shifted - (64 * x + 32 * z + 4 + 4 * i)) & 127) < 4
                for h in range(2):
                    outs[n][h] = jnp.where(m, us[h], outs[n][h])
        for n, (x, z) in enumerate(quads):
            for h in range(2):
                res_tx[x, z, h] = roll(outs[n][h], lax.rem(120 * gz + 256 - (64 * x + 32 * z + 4), 128))
        for h in range(2):
            res_rx[gz, h] = res_tx[0, gz, h]

    def res_copy(x, z):
        return remote(res_tx.at[x, z], res_rx.at[gz], e_sem.at[x, z, 0], e_sem.at[2, gz, 0], (z, x, gy))

    def main_problem():
        pass_cp.start()
        own_near.start()
        with jax.named_scope("fac1"):
            main_factors(1)
        with jax.named_scope("wait_lc"):
            raw_cp[LC].wait_recv()
        with jax.named_scope("fac0m"):
            main_factors(0)
        g_cp.start()
        with jax.named_scope("wait_raw"):
            for a in (U, PC, SRC):
                raw_cp[a].wait_recv()
        with jax.named_scope("f0"):
            forward_main(0)
        own_far.start()
        with jax.named_scope("wait_g"):
            g_cp.wait()
        for k in range(HALF):
            for t in range(2):
                g = gtx[t, k]
                mid[1, k, t] = 1.0 / ((g + grx[t, k] * (1.0 - g)) * prv[k, t, zof(NJ - 1)])
        for k in range(1, HALF):
            with jax.named_scope(f"w{k - 1}"):
                wait_d(k - 1)
            with jax.named_scope(f"b{k - 1}"):
                backward_main(k - 1)
            with jax.named_scope(f"f{k}"):
                forward_main(k)
        dsc_cp.start()
        fin[0] = dtx[HALF - 1, 0] * mid[1, HALF - 1, 0]
        fin[1] = (1.0 - gtx[0, HALF - 1]) * mid[1, HALF - 1, 0]
        fin_cp.start()

    def edge_problem():
        for a in range(4):
            for g in range(4):
                own_rx[gx, gz, a, g] = own_pk[gz, a, g]
        with jax.named_scope("fac0"):
            main_factors(0)
        with jax.named_scope("wait_own"):
            for x, z in quads:

                @pl.when((x == 1) | (z != gz))
                def _():
                    remote(own_rx.at[x, z], own_rx.at[x, z], own_sem.at[0, 0, 0], own_sem.at[1, x, z], (gz, 1, gy)).wait_recv()

        with jax.named_scope("unpack_own"):
            unpack_own()

        @pl.when(((gz == 0) & has_left) | ((gz == 1) & has_right))
        def _():
            with jax.named_scope("wait_halo"):
                for x, z in quads:
                    remote(halo_rx.at[x, z], halo_rx.at[x, z], halo_sem.at[0, 0, 0], halo_sem.at[1, x, z], (gz, 1, gy)).wait_recv()
            with jax.named_scope("unpack_halo"):
                unpack_halo()

        with jax.named_scope("edge_fac"):
            edge_factors()
        for k in range(HALF):
            with jax.named_scope(f"e{k}"):
                edge_step(k)
        with jax.named_scope("epack"):
            pack_result()
        for x, z in ((1, 0), (1, 1), (0, 0), (0, 1)):

            @pl.when((x == 1) | (z != gz))
            def _():
                res_copy(x, z).start()

    @pl.when(gx == 1)
    def _():
        main_problem()

    @pl.when(gx == 0)
    def _():
        with jax.named_scope("wait_y"):
            pl.semaphore_wait(barrier, has_left.astype(jnp.int32) + has_right.astype(jnp.int32))
        for x in range(2):
            if x:
                with jax.named_scope("wait_pass"):
                    pass_cp.wait_recv()
            for side, there in enumerate((has_left, has_right)):
                pl.when(there)(halo_copy(x, side).start)
        own_far.start()
        edge_problem()

    with jax.named_scope("we"):
        for side in range(2):

            @pl.when((gx == 1) | (gz != side))
            def _():
                remote(res_rx.at[side], res_rx.at[side], e_sem.at[0, 0, 0], e_sem.at[2, side, 0], (gz, 1 - gx, gy)).wait_recv()

    first, last = lane < 4, lane >= 124

    def finish(t, y):
        k = HALF - 1
        for j in reversed(range(NJ)):
            z, at = zof(j), (-4 * (j % 32)) % 128
            left, right = res_rx[0, j // 32], res_rx[1, j // 32]
            if at:
                left, right = roll(left, at), roll(right, at)
            if j < NJ - 1:
                y = y + dsc[t, z] * quo[k, t, z]
            out_ref[z] = jnp.where(last, right, jnp.where(first, left, prv[k, t, z] * y))

    @pl.when(gx == 1)
    def _():
        k = HALF - 1
        with jax.named_scope("w3"):
            wait_d(k)
        with jax.named_scope("finish"):
            finish(1, (dtx[k, 1] + (1.0 - gtx[1, k]) * drx[k, 1]) * mid[1, k, 1])
        pass_cp.wait_send()
        own_near.wait_send()
        for i in range(HALF):
            d_copy(i).wait_send()
        last_copy.wait_send()
        dsc_cp.wait_send()
        fin_cp.wait_send()

    @pl.when(gx == 0)
    def _():
        with jax.named_scope("w3s"):
            dsc_cp.wait_recv()
            fin_cp.wait_recv()
            last_copy.wait_recv()
        with jax.named_scope("finish_s"):
            finish(0, fin_rx[0] + fin_rx[1] * drx[HALF - 1, 0])
        for c in raw_cp.values():
            c.wait_send()
        for x, z in quads:

            @pl.when((x == 1) | (z != gz))
            def _():
                res_copy(x, z).wait_send()

        for x in range(2):
            for side, there in enumerate((has_left, has_right)):
                pl.when(there)(halo_copy(x, side).wait_send)

    own_far.wait_send()


def solution(mesh):
    ny = mesh.shape["gy"]
    block = (NJ, 8, 128)
    vmem = lambda *s: pltpu.VMEM((*s, 8, 128), jnp.float32)

    def on_device(u, pc, lc, src, table, rows):
        hbm = pl.BlockSpec(memory_space=pltpu.HBM)
        args = [pltpu.with_memory_space_constraint(x, pltpu.HBM) for x in (u, pc, lc, src, table, rows)]
        return pl.pallas_call(
            functools.partial(kernel, ny),
            out_shape=jax.ShapeDtypeStruct(block, jnp.float32),
            in_specs=[hbm] * 6,
            out_specs=pl.BlockSpec(memory_space=pltpu.VMEM),
            scratch_shapes=[
                vmem(4, 2, NJ),
                vmem(HALF, 2, NJ), vmem(HALF, 2, NJ), vmem(HALF, 2, NJ),
                vmem(2, NJ), vmem(2, HALF, 2),
                vmem(2, HALF), vmem(2, HALF), vmem(HALF, 2), vmem(HALF, 2),
                vmem(2, 4, 4), vmem(2, 2, 4, 4), vmem(2, 4, 2), vmem(2, 2, 4, 2),
                vmem(4, NJ), vmem(HALF, NJ), vmem(HALF, NJ), vmem(HALF, NJ),
                vmem(NJ), vmem(2, HALF), vmem(2, 2, 2), vmem(2, 2), vmem(2, 4, 2), vmem(2), vmem(2),
                pltpu.SMEM((8,), jnp.float32), pltpu.SMEM((HALF,), jnp.int32),
                pltpu.SemaphoreType.DMA((6,)),
                pltpu.SemaphoreType.DMA((2, 4)),
                pltpu.SemaphoreType.DMA((2, 2, 2)),
                pltpu.SemaphoreType.DMA((2, 2, 2)),
                pltpu.SemaphoreType.DMA((2,)),
                pltpu.SemaphoreType.DMA((2,)),
                pltpu.SemaphoreType.DMA((2, HALF)),
                pltpu.SemaphoreType.DMA((2,)),
                pltpu.SemaphoreType.DMA((2, 2)),
                pltpu.SemaphoreType.DMA((3, 2, 1)),
                pltpu.SemaphoreType.REGULAR,
            ],
            compiler_params=pltpu.CompilerParams(collective_id=0, has_side_effects=True, vmem_limit_bytes=24 * 2**20),
        )(*args)

    split = P("gz", "gx", "gy")
    return jax.shard_map(
        on_device, mesh=mesh, in_specs=(split,) * 4 + (P(), P()), out_specs=split, check_vma=False
    )
```

```python
import functools

import jax
import jax.numpy as jnp
from jax import lax
from jax.experimental import pallas as pl
from jax.experimental.pallas import tpu as pltpu
from jax.sharding import PartitionSpec as P

HALF = 4
NJ = 64
MESH = pl.DeviceIdType.MESH
U, PC, SRC, LC = range(4)
LC_FILL = 4000.0


def kernel(
    ny,
    u_hbm, pc_hbm, lc_hbm, src_hbm, table_hbm, rows_hbm,
    out_ref,
    raw, fac, prv, quo, dsc, mid, gtx, grx, dtx, drx,
    own_pk, own_rx, halo_pk, halo_rx, est, efac, eprv, equo, eds, emid, res_tx, res_rx, pass_rx, fin, fin_rx,
    table, rows, load_sem, raw_sem, own_sem, halo_sem, pass_sem, g_sem, d_sem, last_sem, fin_sem, e_sem, go,
):
    gz, gx, gy = lax.axis_index("gz"), lax.axis_index("gx"), lax.axis_index("gy")
    has_left, has_right = gy > 0, gy < ny - 1
    y_left, y_right = lax.rem(gy + ny - 1, ny), lax.rem(gy + 1, ny)
    lane = lax.broadcasted_iota(jnp.int32, (8, 128), 1)
    row = lax.broadcasted_iota(jnp.int32, (8, 128), 0)
    base = 64 * gx + 32 * gz
    ones = jnp.full((8, 128), 1.0, jnp.float32)
    zero = jnp.zeros((8, 128), jnp.float32)

    half = [0]

    def zof(j):
        return NJ - 1 - j if half[0] else j

    def each_half(f):
        for z in range(2):

            @pl.when(gz == z)
            def _():
                half[0] = z
                f()


    def remote(src, dst, send, recv, dev):
        return pltpu.make_async_remote_copy(
            src_ref=src, dst_ref=dst, send_sem=send, recv_sem=recv, device_id=dev, device_id_type=MESH
        )

    def roll(v, amount, axis=1):
        return pltpu.roll(v, amount, axis)

    loads = [
        pltpu.make_async_copy(ref, raw.at[a, gx], load_sem.at[a])
        for a, ref in ((LC, lc_hbm), (U, u_hbm), (PC, pc_hbm), (SRC, src_hbm))
    ]
    loads.append(pltpu.make_async_copy(table_hbm, table, load_sem.at[4]))
    loads.append(pltpu.make_async_copy(rows_hbm, rows, load_sem.at[5]))
    for c in loads:
        c.start()
    barrier = pltpu.get_barrier_semaphore()

    def hello(sem, dev):
        pl.semaphore_signal(sem, inc=1, device_id=dev, device_id_type=MESH)

    hello(barrier, (1 - gz, 1, gy))

    @pl.when(gx == 0)
    def _():
        hello(barrier, (gz, 1, gy))

    @pl.when((gx == 0) & (gz == 0) & has_left)
    def _():
        for z in range(2):
            hello(barrier, (z, 0, y_left))

    @pl.when((gx == 0) & (gz == 1) & has_right)
    def _():
        for z in range(2):
            hello(barrier, (z, 0, y_right))

    with jax.named_scope("wait_barrier"):

        @pl.when(gx == 1)
        def _():
            pl.semaphore_wait(barrier, 3)
            hello(go, (gz, 0, gy))

        @pl.when(gx == 0)
        def _():
            pl.semaphore_wait(go, 1)

    for c in loads:
        c.wait()

    raw_cp = {
        a: remote(raw.at[a, 0], raw.at[a, 0], raw_sem.at[0, a], raw_sem.at[1, a], (gz, 1, gy)) for a in (LC, U, PC, SRC)
    }

    @pl.when(gx == 0)
    def _():
        for c in raw_cp.values():
            c.start()


    spot = (lane - base - 4) & 127
    low_half, even = (spot & 7) < 4, (spot & 8) == 0
    group = jnp.where(gz == 0, spot >> 4, 7 - (spot >> 4))
    places = [(base + 12 + jnp.where(gz == 0, 16 * b, 112 - 16 * b)) & 127 for b in range(8)]
    forwards = jnp.full((8, 128), gz, jnp.int32) == 0

    def in_order(pair):
        return jnp.where(forwards, pair[0], pair[1]), jnp.where(forwards, pair[1], pair[0])

    def pack(g, _):
        at = jnp.where(gz == 0, g, 1 - g)
        for a in range(4):
            left, right = [], []
            for h in range(2):
                both = []
                for q in range(2):
                    v = zero
                    for b in range(8):
                        w = roll(raw[a, gx, g * 32 + (h * 16 + q * 8 + b)], places[b])
                        v = w if b == 0 else jnp.where(group == b, w, v)
                    both.append(v)
                both = in_order(both)
                left.append(jnp.where(even, roll(both[0], 120), both[1]))
                right.append(jnp.where(even, both[0], roll(both[1], 8)))
            left, right = in_order(left), in_order(right)
            for h in range(2):
                own_pk[0, a, 2 * at + h] = left[h]
                own_pk[1, a, 2 * at + h] = right[h]
            halo_pk[0, a, at] = jnp.where(low_half, roll(left[0], 8), roll(left[1], 12))
            halo_pk[1, a, at] = jnp.where(low_half, roll(right[1], 124), roll(right[0], 120))
        return 0

    def octet(jj):
        return 8 * (2 * jj if jj < 8 else 2 * (jj - 8) + 1)

    with jax.named_scope("pack"):
        lax.fori_loop(0, 2, pack, 0)

    pass_cp = remote(halo_pk, pass_rx, pass_sem.at[0], pass_sem.at[1], (gz, 0, gy))

    def halo_copy(x, side):
        pk, dev = (halo_pk, pass_rx)[x], ((1, 0, y_left), (0, 0, y_right))[side]
        return remote(pk.at[side], halo_rx.at[x, gz], halo_sem.at[0, side, x], halo_sem.at[1, x, gz], dev)

    own_far = remote(own_pk.at[1 - gz], own_rx.at[gx, gz], own_sem.at[0, 0, 0], own_sem.at[1, gx, gz], (1 - gz, 0, gy))
    own_near = remote(own_pk.at[gz], own_rx.at[1, gz], own_sem.at[0, 0, 1], own_sem.at[1, 1, gz], (gz, 0, gy))
    g_cp = remote(gtx, grx, g_sem.at[0], g_sem.at[1], (1 - gz, 1, gy))

    def d_copy(k):
        return remote(dtx.at[k], drx.at[k], d_sem.at[0, k], d_sem.at[1, k], (1 - gz, 1, gy))

    def wait_d(k):
        d_copy(k).wait_recv()

    last_copy = remote(dtx.at[HALF - 1, 0], drx.at[HALF - 1, 0], last_sem.at[0], last_sem.at[1], (1 - gz, 0, gy))
    dsc_cp = remote(dsc.at[0], dsc.at[0], fin_sem.at[0, 0], fin_sem.at[1, 0], (gz, 0, gy))
    fin_cp = remote(fin, fin_rx, fin_sem.at[0, 1], fin_sem.at[1, 1], (gz, 0, gy))

    inv = []
    for k in range(HALF):
        shift = jnp.float32(0.0)
        for i in range(table.shape[0]):
            shift = shift + jnp.where(rows[k] == i, table[i], 0.0)
        inv.append(1.0 / jnp.full((8, 128), shift, jnp.float32))

    def factors(load_lc, store):
        def block(b, carry):
            ps, ds, rs = carry
            ps, ds, rs = list(ps), list(ds), list(rs)
            for i in range(16):
                j = b * 16 + i
                t_line = 1.0 / load_lc(j)
                for k in range(HALF):
                    old, r_old = ps[k], rs[k]
                    ds[k] = ds[k] + (t_line * inv[k]) * old
                    ps[k] = old + ds[k]
                    rs[k] = 1.0 / ps[k]
                    store(k, j, t_line * old, old, r_old * rs[k])
            return tuple(ps), tuple(ds), tuple(rs)

        start = (ones,) * HALF
        return lax.fori_loop(0, NJ // 16, block, (start, start, start))

    def main_factors(t):
        def store(k, j, f, p, q):
            z = zof(j)
            fac[k, t, z] = f
            prv[k, t, z] = p
            quo[k, t, z] = q

        ps, ds, rs = factors(lambda j: raw[LC, t, zof(j)], store)
        for k in range(HALF):
            mid[0, k, t] = rs[k]
            gtx[t, k] = ds[k] * rs[k]

    def forward_main(k):
        def block(b, totals):
            totals = list(totals)
            for i in range(64):
                z = zof(i)
                us = [raw[U, 0, z], raw[U, 1, z]]
                down = [roll(u, 1, 0) for u in us]
                up = [roll(u, 7, 0) for u in us]
                low = [jnp.where(row == 0, 0.0, down[0]), jnp.where(row == 0, down[0], down[1])]
                high = [jnp.where(row == 7, up[1], up[0]), jnp.where(row == 7, 0.0, up[1])]
                for t in range(2):
                    beside = (low[t] + high[t]) + (roll(us[t], 1) + roll(us[t], 127))
                    e = inv[k] * us[t] + raw[PC, t, z] * (beside - 4.0 * us[t]) + raw[SRC, t, z]
                    totals[t] = totals[t] + fac[k, t, z] * e
                    dsc[t, z] = totals[t]
            return tuple(totals)

        totals = block(0, (zero, zero))
        for t in range(2):
            dtx[k, t] = totals[t] * mid[0, k, t]
        d_copy(k).start()
        if k == HALF - 1:
            last_copy.start()

    def backward_main(k):
        last = zof(NJ - 1)
        ys = []
        for t in range(2):
            y = (dtx[k, t] + (1.0 - gtx[t, k]) * drx[k, t]) * mid[1, k, t]
            raw[U, t, last] = prv[k, t, last] * y
            ys.append(y)

        for j in reversed(range(NJ - 1)):
            z = zof(j)
            for t in range(2):
                ys[t] = ys[t] + dsc[t, z] * quo[k, t, z]
                raw[U, t, z] = prv[k, t, z] * ys[t]

    quads = [(x, z) for x in range(2) for z in range(2)]
    fills = {U: 0.0, PC: 0.0, SRC: 0.0, LC: LC_FILL}

    def unpack_own():
        def block(g, _):
            for jj in range(16):
                masks = [((lane - (64 * x + 32 * z + 4 + octet(jj))) & 127) < 8 for x, z in quads]
                for a in range(4):
                    v = jnp.full((8, 128), fills[a], jnp.float32)
                    for (x, z), m in zip(quads, masks):
                        v = jnp.where(m, own_rx[x, z, a, g], v)
                    est[a, g * 16 + jj] = roll(v, (-octet(jj)) % 128) if jj else v
            return 0

        lax.fori_loop(0, 4, block, 0)

    def unpack_halo():
        shifted = lane - 12 * gz

        def block(g, _):
            for jj in range(32):
                at = octet(jj) if jj < 16 else octet(jj - 16) + 4
                masks = [((shifted - (64 * x + 32 * z + at)) & 127) < 4 for x, z in quads]
                m_all = (shifted & 31) < 4
                for a in range(4):
                    v = zero
                    for (x, z), m in zip(quads, masks):
                        v = jnp.where(m, halo_rx[x, z, a, g], v)
                    v = roll(v, (-at) % 128) if at else v
                    est[a, g * 32 + jj] = jnp.where(m_all, v, est[a, g * 32 + jj])
            return 0

        lax.fori_loop(0, 2, block, 0)

    def edge_factors():
        def store(k, j, f, p, q):
            efac[k, j] = f
            eprv[k, j] = p
            equo[k, j] = q

        ps, ds, rs = factors(lambda j: est[LC, j], store)
        for k in range(HALF):
            emid[0, k] = ds[k] * rs[k]
            emid[1, k] = rs[k]

    def other_half(v):
        return jnp.where((lane & 32) == 0, roll(v, 96), roll(v, 32))

    def edge_step(k):
        outer_low = (row == 0) & (lane < 64)
        outer_high = (row == 7) & (lane >= 64)

        def fwd(b, total):
            for i in range(64):
                j = i
                u = est[U, j]
                cross = roll(u, 64)
                low = jnp.where(outer_low, 0.0, roll(jnp.where(row == 7, cross, u), 1, 0))
                high = jnp.where(outer_high, 0.0, roll(jnp.where(row == 0, cross, u), 7, 0))
                beside = (low + high) + (roll(u, 1) + roll(u, 127))
                e = inv[k] * u + est[PC, j] * (beside - 4.0 * u) + est[SRC, j]
                total = total + efac[k, j] * e
                eds[j] = total
            return total

        total = fwd(0, zero)
        d = total * emid[1, k]
        g = emid[0, k]
        last_p = eprv[k, NJ - 1]
        y = (d + (1.0 - g) * other_half(d)) / ((g + other_half(g) * (1.0 - g)) * last_p)
        est[U, NJ - 1] = last_p * y

        for j in reversed(range(NJ - 1)):
            y = y + eds[j] * equo[k, j]
            est[U, j] = eprv[k, j] * y

    def pack_result():
        shifted = lane - 4 * gz
        outs = [[zero, zero] for _ in quads]
        for i in range(32):
            us = [est[U, i], est[U, 32 + i]]
            if i:
                us = [roll(u, 4 * i) for u in us]
            for n, (x, z) in enumerate(quads):
                m = ((shifted - (64 * x + 32 * z + 4 + 4 * i)) & 127) < 4
                for h in range(2):
                    outs[n][h] = jnp.where(m, us[h], outs[n][h])
        for n, (x, z) in enumerate(quads):
            for h in range(2):
                res_tx[x, z, h] = roll(outs[n][h], lax.rem(120 * gz + 256 - (64 * x + 32 * z + 4), 128))
        for h in range(2):
            res_rx[gz, h] = res_tx[0, gz, h]

    def res_copy(x, z):
        return remote(res_tx.at[x, z], res_rx.at[gz], e_sem.at[x, z, 0], e_sem.at[2, gz, 0], (z, x, gy))

    def main_problem():
        pass_cp.start()
        own_near.start()
        with jax.named_scope("fac1"):
            main_factors(1)
        with jax.named_scope("wait_lc"):
            raw_cp[LC].wait_recv()
        with jax.named_scope("fac0m"):
            main_factors(0)
        g_cp.start()
        with jax.named_scope("wait_raw"):
            for a in (U, PC, SRC):
                raw_cp[a].wait_recv()
        with jax.named_scope("f0"):
            forward_main(0)
        own_far.start()
        with jax.named_scope("wait_g"):
            g_cp.wait()
        for k in range(HALF):
            for t in range(2):
                g = gtx[t, k]
                mid[1, k, t] = 1.0 / ((g + grx[t, k] * (1.0 - g)) * prv[k, t, zof(NJ - 1)])
        for k in range(1, HALF):
            with jax.named_scope(f"w{k - 1}"):
                wait_d(k - 1)
            with jax.named_scope(f"b{k - 1}"):
                backward_main(k - 1)
            with jax.named_scope(f"f{k}"):
                forward_main(k)
        dsc_cp.start()
        fin[0] = dtx[HALF - 1, 0] * mid[1, HALF - 1, 0]
        fin[1] = (1.0 - gtx[0, HALF - 1]) * mid[1, HALF - 1, 0]
        fin_cp.start()

    def edge_problem():
        for a in range(4):
            for g in range(4):
                own_rx[gx, gz, a, g] = own_pk[gz, a, g]
        with jax.named_scope("fac0"):
            each_half(lambda: main_factors(0))
        with jax.named_scope("wait_own"):
            for x, z in quads:

                @pl.when((x == 1) | (z != gz))
                def _():
                    remote(own_rx.at[x, z], own_rx.at[x, z], own_sem.at[0, 0, 0], own_sem.at[1, x, z], (gz, 1, gy)).wait_recv()

        with jax.named_scope("unpack_own"):
            unpack_own()

        @pl.when(((gz == 0) & has_left) | ((gz == 1) & has_right))
        def _():
            with jax.named_scope("wait_halo"):
                for x, z in quads:
                    remote(halo_rx.at[x, z], halo_rx.at[x, z], halo_sem.at[0, 0, 0], halo_sem.at[1, x, z], (gz, 1, gy)).wait_recv()
            with jax.named_scope("unpack_halo"):
                unpack_halo()

        with jax.named_scope("edge_fac"):
            edge_factors()
        for k in range(HALF):
            with jax.named_scope(f"e{k}"):
                edge_step(k)
        with jax.named_scope("epack"):
            pack_result()
        for x, z in ((1, 0), (1, 1), (0, 0), (0, 1)):

            @pl.when((x == 1) | (z != gz))
            def _():
                res_copy(x, z).start()

    @pl.when(gx == 1)
    def _():
        each_half(main_problem)

    @pl.when(gx == 0)
    def _():
        with jax.named_scope("wait_y"):
            pl.semaphore_wait(barrier, has_left.astype(jnp.int32) + has_right.astype(jnp.int32))
        for x in range(2):
            if x:
                with jax.named_scope("wait_pass"):
                    pass_cp.wait_recv()
            for side, there in enumerate((has_left, has_right)):
                pl.when(there)(halo_copy(x, side).start)
        own_far.start()
        edge_problem()

    with jax.named_scope("we"):
        for side in range(2):

            @pl.when((gx == 1) | (gz != side))
            def _():
                remote(res_rx.at[side], res_rx.at[side], e_sem.at[0, 0, 0], e_sem.at[2, side, 0], (gz, 1 - gx, gy)).wait_recv()

    first, last = lane < 4, lane >= 124

    def finish(t, y):
        k = HALF - 1
        for j in reversed(range(NJ)):
            z, at = zof(j), (-4 * (j % 32)) % 128
            left, right = res_rx[0, j // 32], res_rx[1, j // 32]
            if at:
                left, right = roll(left, at), roll(right, at)
            if j < NJ - 1:
                y = y + dsc[t, z] * quo[k, t, z]
            out_ref[z] = jnp.where(last, right, jnp.where(first, left, prv[k, t, z] * y))

    @pl.when(gx == 1)
    def _():
        k = HALF - 1
        with jax.named_scope("w3"):
            wait_d(k)
        with jax.named_scope("finish"):
            each_half(lambda: finish(1, (dtx[k, 1] + (1.0 - gtx[1, k]) * drx[k, 1]) * mid[1, k, 1]))
        pass_cp.wait_send()
        own_near.wait_send()
        for i in range(HALF):
            d_copy(i).wait_send()
        last_copy.wait_send()
        dsc_cp.wait_send()
        fin_cp.wait_send()

    @pl.when(gx == 0)
    def _():
        with jax.named_scope("w3s"):
            dsc_cp.wait_recv()
            fin_cp.wait_recv()
            last_copy.wait_recv()
        with jax.named_scope("finish_s"):
            each_half(lambda: finish(0, fin_rx[0] + fin_rx[1] * drx[HALF - 1, 0]))
        for c in raw_cp.values():
            c.wait_send()
        for x, z in quads:

            @pl.when((x == 1) | (z != gz))
            def _():
                res_copy(x, z).wait_send()

        for x in range(2):
            for side, there in enumerate((has_left, has_right)):
                pl.when(there)(halo_copy(x, side).wait_send)

    own_far.wait_send()


def solution(mesh):
    ny = mesh.shape["gy"]
    block = (NJ, 8, 128)
    vmem = lambda *s: pltpu.VMEM((*s, 8, 128), jnp.float32)

    def on_device(u, pc, lc, src, table, rows):
        hbm = pl.BlockSpec(memory_space=pltpu.HBM)
        args = [pltpu.with_memory_space_constraint(x, pltpu.HBM) for x in (u, pc, lc, src, table, rows)]
        return pl.pallas_call(
            functools.partial(kernel, ny),
            out_shape=jax.ShapeDtypeStruct(block, jnp.float32),
            in_specs=[hbm] * 6,
            out_specs=pl.BlockSpec(memory_space=pltpu.VMEM),
            scratch_shapes=[
                vmem(4, 2, NJ),
                vmem(HALF, 2, NJ), vmem(HALF, 2, NJ), vmem(HALF, 2, NJ),
                vmem(2, NJ), vmem(2, HALF, 2),
                vmem(2, HALF), vmem(2, HALF), vmem(HALF, 2), vmem(HALF, 2),
                vmem(2, 4, 4), vmem(2, 2, 4, 4), vmem(2, 4, 2), vmem(2, 2, 4, 2),
                vmem(4, NJ), vmem(HALF, NJ), vmem(HALF, NJ), vmem(HALF, NJ),
                vmem(NJ), vmem(2, HALF), vmem(2, 2, 2), vmem(2, 2), vmem(2, 4, 2), vmem(2), vmem(2),
                pltpu.SMEM((8,), jnp.float32), pltpu.SMEM((HALF,), jnp.int32),
                pltpu.SemaphoreType.DMA((6,)),
                pltpu.SemaphoreType.DMA((2, 4)),
                pltpu.SemaphoreType.DMA((2, 2, 2)),
                pltpu.SemaphoreType.DMA((2, 2, 2)),
                pltpu.SemaphoreType.DMA((2,)),
                pltpu.SemaphoreType.DMA((2,)),
                pltpu.SemaphoreType.DMA((2, HALF)),
                pltpu.SemaphoreType.DMA((2,)),
                pltpu.SemaphoreType.DMA((2, 2)),
                pltpu.SemaphoreType.DMA((3, 2, 1)),
                pltpu.SemaphoreType.REGULAR,
            ],
            compiler_params=pltpu.CompilerParams(collective_id=0, has_side_effects=True, vmem_limit_bytes=24 * 2**20),
        )(*args)

    split = P("gz", "gx", "gy")
    return jax.shard_map(
        on_device, mesh=mesh, in_specs=(split,) * 4 + (P(), P()), out_specs=split, check_vma=False
    )
```

```python
import functools

import jax
import jax.numpy as jnp
from jax import lax
from jax.experimental import pallas as pl
from jax.experimental.pallas import tpu as pltpu
from jax.sharding import PartitionSpec as P

HALF = 4
NJ = 64
MESH = pl.DeviceIdType.MESH
U, PC, SRC, LC = range(4)
LC_FILL = 4000.0


def kernel(
    ny,
    u_hbm, pc_hbm, lc_hbm, src_hbm, table_hbm, rows_hbm,
    out_ref,
    raw, fac, prv, quo, dsc, mid, gtx, grx, dtx, drx,
    own_pk, own_rx, halo_pk, halo_rx, est, efac, eprv, equo, eds, emid, res_tx, res_rx, pass_rx, fin, fin_rx,
    table, rows, load_sem, raw_sem, own_sem, halo_sem, pass_sem, g_sem, d_sem, last_sem, fin_sem, e_sem, go,
):
    gz, gx, gy = lax.axis_index("gz"), lax.axis_index("gx"), lax.axis_index("gy")
    has_left, has_right = gy > 0, gy < ny - 1
    y_left, y_right = lax.rem(gy + ny - 1, ny), lax.rem(gy + 1, ny)
    lane = lax.broadcasted_iota(jnp.int32, (8, 128), 1)
    row = lax.broadcasted_iota(jnp.int32, (8, 128), 0)
    base = 64 * gx + 32 * gz
    ones = jnp.full((8, 128), 1.0, jnp.float32)
    zero = jnp.zeros((8, 128), jnp.float32)

    half = [0]

    def zof(j):
        return NJ - 1 - j if half[0] else j

    def each_half(f):
        for z in range(2):

            @pl.when(gz == z)
            def _():
                half[0] = z
                f()


    def remote(src, dst, send, recv, dev):
        return pltpu.make_async_remote_copy(
            src_ref=src, dst_ref=dst, send_sem=send, recv_sem=recv, device_id=dev, device_id_type=MESH
        )

    def roll(v, amount, axis=1):
        return pltpu.roll(v, amount, axis)

    loads = [
        pltpu.make_async_copy(ref, raw.at[a, gx], load_sem.at[a])
        for a, ref in ((LC, lc_hbm), (U, u_hbm), (PC, pc_hbm), (SRC, src_hbm))
    ]
    loads.append(pltpu.make_async_copy(table_hbm, table, load_sem.at[4]))
    loads.append(pltpu.make_async_copy(rows_hbm, rows, load_sem.at[5]))
    for c in loads:
        c.start()
    barrier = pltpu.get_barrier_semaphore()

    def hello(sem, dev):
        pl.semaphore_signal(sem, inc=1, device_id=dev, device_id_type=MESH)

    hello(barrier, (1 - gz, 1, gy))

    @pl.when(gx == 0)
    def _():
        hello(barrier, (gz, 1, gy))

    @pl.when((gx == 0) & (gz == 0) & has_left)
    def _():
        for z in range(2):
            hello(barrier, (z, 0, y_left))

    @pl.when((gx == 0) & (gz == 1) & has_right)
    def _():
        for z in range(2):
            hello(barrier, (z, 0, y_right))

    with jax.named_scope("wait_barrier"):

        @pl.when(gx == 1)
        def _():
            pl.semaphore_wait(barrier, 3)
            hello(go, (gz, 0, gy))

        @pl.when(gx == 0)
        def _():
            pl.semaphore_wait(go, 1)

    for c in loads:
        c.wait()

    raw_cp = {
        a: remote(raw.at[a, 0], raw.at[a, 0], raw_sem.at[0, a], raw_sem.at[1, a], (gz, 1, gy)) for a in (LC, U, PC, SRC)
    }

    @pl.when(gx == 0)
    def _():
        for c in raw_cp.values():
            c.start()


    spot = (lane - base - 4) & 127
    low_half, even = (spot & 7) < 4, (spot & 8) == 0
    group = jnp.where(gz == 0, spot >> 4, 7 - (spot >> 4))
    places = [(base + 12 + jnp.where(gz == 0, 16 * b, 112 - 16 * b)) & 127 for b in range(8)]
    forwards = jnp.full((8, 128), gz, jnp.int32) == 0

    def in_order(pair):
        return jnp.where(forwards, pair[0], pair[1]), jnp.where(forwards, pair[1], pair[0])

    def pack(g, _):
        at = jnp.where(gz == 0, g, 1 - g)
        for a in range(4):
            left, right = [], []
            for h in range(2):
                both = []
                for q in range(2):
                    v = zero
                    for b in range(8):
                        w = roll(raw[a, gx, g * 32 + (h * 16 + q * 8 + b)], places[b])
                        v = w if b == 0 else jnp.where(group == b, w, v)
                    both.append(v)
                both = in_order(both)
                left.append(jnp.where(even, roll(both[0], 120), both[1]))
                right.append(jnp.where(even, both[0], roll(both[1], 8)))
            left, right = in_order(left), in_order(right)
            for h in range(2):
                own_pk[0, a, 2 * at + h] = left[h]
                own_pk[1, a, 2 * at + h] = right[h]
            halo_pk[0, a, at] = jnp.where(low_half, roll(left[0], 8), roll(left[1], 12))
            halo_pk[1, a, at] = jnp.where(low_half, roll(right[1], 124), roll(right[0], 120))
        return 0

    def octet(jj):
        return 8 * (2 * jj if jj < 8 else 2 * (jj - 8) + 1)

    with jax.named_scope("pack"):
        lax.fori_loop(0, 2, pack, 0)

    pass_cp = remote(halo_pk, pass_rx, pass_sem.at[0], pass_sem.at[1], (gz, 0, gy))

    pieces = ((LC, 1), (0, 3))

    def halo_copy(x, side, piece):
        pk, dev = (halo_pk, pass_rx)[x], ((1, 0, y_left), (0, 0, y_right))[side]
        part, sem = pl.ds(*pieces[piece]), halo_sem.at[piece]
        return remote(pk.at[side, part], halo_rx.at[x, gz, part], sem.at[0, side, x], sem.at[1, x, gz], dev)

    own_far = remote(own_pk.at[1 - gz], own_rx.at[gx, gz], own_sem.at[0, 0, 0], own_sem.at[1, gx, gz], (1 - gz, 0, gy))
    own_near = remote(own_pk.at[gz], own_rx.at[1, gz], own_sem.at[0, 0, 1], own_sem.at[1, 1, gz], (gz, 0, gy))
    g_cp = remote(gtx, grx, g_sem.at[0], g_sem.at[1], (1 - gz, 1, gy))

    def d_copy(k):
        return remote(dtx.at[k], drx.at[k], d_sem.at[0, k], d_sem.at[1, k], (1 - gz, 1, gy))

    def wait_d(k):
        d_copy(k).wait_recv()

    last_copy = remote(dtx.at[HALF - 1, 0], drx.at[HALF - 1, 0], last_sem.at[0], last_sem.at[1], (1 - gz, 0, gy))
    dsc_cp = remote(dsc.at[0], dsc.at[0], fin_sem.at[0, 0], fin_sem.at[1, 0], (gz, 0, gy))
    fin_cp = remote(fin, fin_rx, fin_sem.at[0, 1], fin_sem.at[1, 1], (gz, 0, gy))

    inv = []
    for k in range(HALF):
        shift = jnp.float32(0.0)
        for i in range(table.shape[0]):
            shift = shift + jnp.where(rows[k] == i, table[i], 0.0)
        inv.append(1.0 / jnp.full((8, 128), shift, jnp.float32))

    def factors(load_lc, store):
        def block(b, carry):
            ps, ds, rs = carry
            ps, ds, rs = list(ps), list(ds), list(rs)
            for i in range(16):
                j = b * 16 + i
                t_line = 1.0 / load_lc(j)
                for k in range(HALF):
                    old, r_old = ps[k], rs[k]
                    ds[k] = ds[k] + (t_line * inv[k]) * old
                    ps[k] = old + ds[k]
                    rs[k] = 1.0 / ps[k]
                    store(k, j, t_line * old, old, r_old * rs[k])
            return tuple(ps), tuple(ds), tuple(rs)

        start = (ones,) * HALF
        return lax.fori_loop(0, NJ // 16, block, (start, start, start))

    def main_factors(t):
        def store(k, j, f, p, q):
            z = zof(j)
            fac[k, t, z] = f
            prv[k, t, z] = p
            quo[k, t, z] = q

        ps, ds, rs = factors(lambda j: raw[LC, t, zof(j)], store)
        for k in range(HALF):
            mid[0, k, t] = rs[k]
            gtx[t, k] = ds[k] * rs[k]

    def forward_main(k):
        def block(b, totals):
            totals = list(totals)
            for i in range(64):
                z = zof(i)
                us = [raw[U, 0, z], raw[U, 1, z]]
                down = [roll(u, 1, 0) for u in us]
                up = [roll(u, 7, 0) for u in us]
                low = [jnp.where(row == 0, 0.0, down[0]), jnp.where(row == 0, down[0], down[1])]
                high = [jnp.where(row == 7, up[1], up[0]), jnp.where(row == 7, 0.0, up[1])]
                for t in range(2):
                    beside = (low[t] + high[t]) + (roll(us[t], 1) + roll(us[t], 127))
                    e = inv[k] * us[t] + raw[PC, t, z] * (beside - 4.0 * us[t]) + raw[SRC, t, z]
                    totals[t] = totals[t] + fac[k, t, z] * e
                    dsc[t, z] = totals[t]
            return tuple(totals)

        totals = block(0, (zero, zero))
        for t in range(2):
            dtx[k, t] = totals[t] * mid[0, k, t]
        d_copy(k).start()
        if k == HALF - 1:
            last_copy.start()

    def backward_main(k):
        last = zof(NJ - 1)
        ys = []
        for t in range(2):
            y = (dtx[k, t] + (1.0 - gtx[t, k]) * drx[k, t]) * mid[1, k, t]
            raw[U, t, last] = prv[k, t, last] * y
            ys.append(y)

        for j in reversed(range(NJ - 1)):
            z = zof(j)
            for t in range(2):
                ys[t] = ys[t] + dsc[t, z] * quo[k, t, z]
                raw[U, t, z] = prv[k, t, z] * ys[t]

    quads = [(x, z) for x in range(2) for z in range(2)]
    fills = {U: 0.0, PC: 0.0, SRC: 0.0, LC: LC_FILL}

    def unpack_own():
        def block(g, _):
            for jj in range(16):
                masks = [((lane - (64 * x + 32 * z + 4 + octet(jj))) & 127) < 8 for x, z in quads]
                for a in range(4):
                    v = jnp.full((8, 128), fills[a], jnp.float32)
                    for (x, z), m in zip(quads, masks):
                        v = jnp.where(m, own_rx[x, z, a, g], v)
                    est[a, g * 16 + jj] = roll(v, (-octet(jj)) % 128) if jj else v
            return 0

        lax.fori_loop(0, 4, block, 0)

    def unpack_halo(arrays):
        shifted = lane - 12 * gz

        def block(g, _):
            for jj in range(32):
                at = octet(jj) if jj < 16 else octet(jj - 16) + 4
                masks = [((shifted - (64 * x + 32 * z + at)) & 127) < 4 for x, z in quads]
                m_all = (shifted & 31) < 4
                for a in arrays:
                    v = zero
                    for (x, z), m in zip(quads, masks):
                        v = jnp.where(m, halo_rx[x, z, a, g], v)
                    v = roll(v, (-at) % 128) if at else v
                    est[a, g * 32 + jj] = jnp.where(m_all, v, est[a, g * 32 + jj])
            return 0

        lax.fori_loop(0, 2, block, 0)

    def edge_factors():
        def store(k, j, f, p, q):
            efac[k, j] = f
            eprv[k, j] = p
            equo[k, j] = q

        ps, ds, rs = factors(lambda j: est[LC, j], store)
        for k in range(HALF):
            emid[0, k] = ds[k] * rs[k]
            emid[1, k] = rs[k]

    def other_half(v):
        return jnp.where((lane & 32) == 0, roll(v, 96), roll(v, 32))

    def edge_step(k):
        outer_low = (row == 0) & (lane < 64)
        outer_high = (row == 7) & (lane >= 64)

        def fwd(b, total):
            for i in range(64):
                j = i
                u = est[U, j]
                cross = roll(u, 64)
                low = jnp.where(outer_low, 0.0, roll(jnp.where(row == 7, cross, u), 1, 0))
                high = jnp.where(outer_high, 0.0, roll(jnp.where(row == 0, cross, u), 7, 0))
                beside = (low + high) + (roll(u, 1) + roll(u, 127))
                e = inv[k] * u + est[PC, j] * (beside - 4.0 * u) + est[SRC, j]
                total = total + efac[k, j] * e
                eds[j] = total
            return total

        total = fwd(0, zero)
        d = total * emid[1, k]
        g = emid[0, k]
        last_p = eprv[k, NJ - 1]
        y = (d + (1.0 - g) * other_half(d)) / ((g + other_half(g) * (1.0 - g)) * last_p)
        est[U, NJ - 1] = last_p * y

        for j in reversed(range(NJ - 1)):
            y = y + eds[j] * equo[k, j]
            est[U, j] = eprv[k, j] * y

    def pack_result():
        shifted = lane - 4 * gz
        outs = [[zero, zero] for _ in quads]
        for i in range(32):
            us = [est[U, i], est[U, 32 + i]]
            if i:
                us = [roll(u, 4 * i) for u in us]
            for n, (x, z) in enumerate(quads):
                m = ((shifted - (64 * x + 32 * z + 4 + 4 * i)) & 127) < 4
                for h in range(2):
                    outs[n][h] = jnp.where(m, us[h], outs[n][h])
        for n, (x, z) in enumerate(quads):
            for h in range(2):
                res_tx[x, z, h] = roll(outs[n][h], lax.rem(120 * gz + 256 - (64 * x + 32 * z + 4), 128))
        for h in range(2):
            res_rx[gz, h] = res_tx[0, gz, h]

    def res_copy(x, z):
        return remote(res_tx.at[x, z], res_rx.at[gz], e_sem.at[x, z, 0], e_sem.at[2, gz, 0], (z, x, gy))

    def main_problem():
        pass_cp.start()
        own_near.start()
        with jax.named_scope("fac1"):
            main_factors(1)
        with jax.named_scope("wait_lc"):
            raw_cp[LC].wait_recv()
        with jax.named_scope("fac0m"):
            main_factors(0)
        g_cp.start()
        with jax.named_scope("wait_raw"):
            for a in (U, PC, SRC):
                raw_cp[a].wait_recv()
        with jax.named_scope("f0"):
            forward_main(0)
        own_far.start()
        with jax.named_scope("wait_g"):
            g_cp.wait()
        for k in range(HALF):
            for t in range(2):
                g = gtx[t, k]
                mid[1, k, t] = 1.0 / ((g + grx[t, k] * (1.0 - g)) * prv[k, t, zof(NJ - 1)])
        for k in range(1, HALF):
            with jax.named_scope(f"w{k - 1}"):
                wait_d(k - 1)
            with jax.named_scope(f"b{k - 1}"):
                backward_main(k - 1)
            with jax.named_scope(f"f{k}"):
                forward_main(k)
        dsc_cp.start()
        fin[0] = dtx[HALF - 1, 0] * mid[1, HALF - 1, 0]
        fin[1] = (1.0 - gtx[0, HALF - 1]) * mid[1, HALF - 1, 0]
        fin_cp.start()

    def edge_problem():
        for a in range(4):
            for g in range(4):
                own_rx[gx, gz, a, g] = own_pk[gz, a, g]
        with jax.named_scope("fac0"):
            each_half(lambda: main_factors(0))
        with jax.named_scope("wait_own"):
            for x, z in quads:

                @pl.when((x == 1) | (z != gz))
                def _():
                    remote(own_rx.at[x, z], own_rx.at[x, z], own_sem.at[0, 0, 0], own_sem.at[1, x, z], (gz, 1, gy)).wait_recv()

        with jax.named_scope("unpack_own"):
            unpack_own()

        def take_halo(piece):
            @pl.when(((gz == 0) & has_left) | ((gz == 1) & has_right))
            def _():
                part = pl.ds(*pieces[piece])
                with jax.named_scope(f"wait_halo{piece}"):
                    for x, z in quads:
                        ref, sem = halo_rx.at[x, z, part], halo_sem.at[piece]
                        remote(ref, ref, sem.at[0, 0, 0], sem.at[1, x, z], (gz, 1, gy)).wait_recv()
                with jax.named_scope(f"unpack_halo{piece}"):
                    unpack_halo(((LC,), (U, PC, SRC))[piece])

        take_halo(0)
        with jax.named_scope("edge_fac"):
            edge_factors()
        take_halo(1)
        for k in range(HALF):
            with jax.named_scope(f"e{k}"):
                edge_step(k)
        with jax.named_scope("epack"):
            pack_result()
        for x, z in ((1, 0), (1, 1), (0, 0), (0, 1)):

            @pl.when((x == 1) | (z != gz))
            def _():
                res_copy(x, z).start()

    @pl.when(gx == 1)
    def _():
        each_half(main_problem)

    @pl.when(gx == 0)
    def _():
        with jax.named_scope("wait_y"):
            pl.semaphore_wait(barrier, has_left.astype(jnp.int32) + has_right.astype(jnp.int32))
        for x in range(2):
            if x:
                with jax.named_scope("wait_pass"):
                    pass_cp.wait_recv()
            for piece in range(2):
                for side, there in enumerate((has_left, has_right)):
                    pl.when(there)(halo_copy(x, side, piece).start)
        own_far.start()
        edge_problem()

    with jax.named_scope("we"):
        for side in range(2):

            @pl.when((gx == 1) | (gz != side))
            def _():
                remote(res_rx.at[side], res_rx.at[side], e_sem.at[0, 0, 0], e_sem.at[2, side, 0], (gz, 1 - gx, gy)).wait_recv()

    first, last = lane < 4, lane >= 124

    def finish(t, y):
        k = HALF - 1
        for j in reversed(range(NJ)):
            z, at = zof(j), (-4 * (j % 32)) % 128
            left, right = res_rx[0, j // 32], res_rx[1, j // 32]
            if at:
                left, right = roll(left, at), roll(right, at)
            if j < NJ - 1:
                y = y + dsc[t, z] * quo[k, t, z]
            out_ref[z] = jnp.where(last, right, jnp.where(first, left, prv[k, t, z] * y))

    @pl.when(gx == 1)
    def _():
        k = HALF - 1
        with jax.named_scope("w3"):
            wait_d(k)
        with jax.named_scope("finish"):
            each_half(lambda: finish(1, (dtx[k, 1] + (1.0 - gtx[1, k]) * drx[k, 1]) * mid[1, k, 1]))
        pass_cp.wait_send()
        own_near.wait_send()
        for i in range(HALF):
            d_copy(i).wait_send()
        last_copy.wait_send()
        dsc_cp.wait_send()
        fin_cp.wait_send()

    @pl.when(gx == 0)
    def _():
        with jax.named_scope("w3s"):
            dsc_cp.wait_recv()
            fin_cp.wait_recv()
            last_copy.wait_recv()
        with jax.named_scope("finish_s"):
            each_half(lambda: finish(0, fin_rx[0] + fin_rx[1] * drx[HALF - 1, 0]))
        for c in raw_cp.values():
            c.wait_send()
        for x, z in quads:

            @pl.when((x == 1) | (z != gz))
            def _():
                res_copy(x, z).wait_send()

        for x in range(2):
            for piece in range(2):
                for side, there in enumerate((has_left, has_right)):
                    pl.when(there)(halo_copy(x, side, piece).wait_send)

    own_far.wait_send()


def solution(mesh):
    ny = mesh.shape["gy"]
    block = (NJ, 8, 128)
    vmem = lambda *s: pltpu.VMEM((*s, 8, 128), jnp.float32)

    def on_device(u, pc, lc, src, table, rows):
        hbm = pl.BlockSpec(memory_space=pltpu.HBM)
        args = [pltpu.with_memory_space_constraint(x, pltpu.HBM) for x in (u, pc, lc, src, table, rows)]
        return pl.pallas_call(
            functools.partial(kernel, ny),
            out_shape=jax.ShapeDtypeStruct(block, jnp.float32),
            in_specs=[hbm] * 6,
            out_specs=pl.BlockSpec(memory_space=pltpu.VMEM),
            scratch_shapes=[
                vmem(4, 2, NJ),
                vmem(HALF, 2, NJ), vmem(HALF, 2, NJ), vmem(HALF, 2, NJ),
                vmem(2, NJ), vmem(2, HALF, 2),
                vmem(2, HALF), vmem(2, HALF), vmem(HALF, 2), vmem(HALF, 2),
                vmem(2, 4, 4), vmem(2, 2, 4, 4), vmem(2, 4, 2), vmem(2, 2, 4, 2),
                vmem(4, NJ), vmem(HALF, NJ), vmem(HALF, NJ), vmem(HALF, NJ),
                vmem(NJ), vmem(2, HALF), vmem(2, 2, 2), vmem(2, 2), vmem(2, 4, 2), vmem(2), vmem(2),
                pltpu.SMEM((8,), jnp.float32), pltpu.SMEM((HALF,), jnp.int32),
                pltpu.SemaphoreType.DMA((6,)),
                pltpu.SemaphoreType.DMA((2, 4)),
                pltpu.SemaphoreType.DMA((2, 2, 2)),
                pltpu.SemaphoreType.DMA((2, 2, 2, 2)),
                pltpu.SemaphoreType.DMA((2,)),
                pltpu.SemaphoreType.DMA((2,)),
                pltpu.SemaphoreType.DMA((2, HALF)),
                pltpu.SemaphoreType.DMA((2,)),
                pltpu.SemaphoreType.DMA((2, 2)),
                pltpu.SemaphoreType.DMA((3, 2, 1)),
                pltpu.SemaphoreType.REGULAR,
            ],
            compiler_params=pltpu.CompilerParams(collective_id=0, has_side_effects=True, vmem_limit_bytes=24 * 2**20),
        )(*args)

    split = P("gz", "gx", "gy")
    return jax.shard_map(
        on_device, mesh=mesh, in_specs=(split,) * 4 + (P(), P()), out_specs=split, check_vma=False
    )
```
